16 devices in a mesh: fsdp: 16 (over z, y, x, core).
Axes of the slice: x: 2, y: 2, z: 2, core: 2. Of those that a mesh axis runs over, the one named last changes fastest.
Arguments:
- x_saved: bfloat16 [2, 32, 1536, 1024], P(None, 'fsdp')
- grad_out: bfloat16 [32, 1536, 1024], P('fsdp')
- x_next: bfloat16 [32, 1536, 1024], P('fsdp')
- w_up: bfloat16 [2, 1024, 4096], replicated
- w_down: bfloat16 [2, 4096, 1024], replicated
- gacc_up: float32 [2, 1024, 4096], P(None, 'fsdp')
- gacc_down: float32 [2, 4096, 1024], P(None, 'fsdp')
- master_up: float32 [2, 1024, 4096], P(None, 'fsdp')
- master_down: float32 [2, 4096, 1024], P(None, 'fsdp')
- mom1_up: float32 [2, 1024, 4096], P(None, 'fsdp')
- mom1_down: float32 [2, 4096, 1024], P(None, 'fsdp')
- mom2_up: float32 [2, 1024, 4096], P(None, 'fsdp')
- mom2_down: float32 [2, 4096, 1024], P(None, 'fsdp')
Outputs:
- output 1: bfloat16 [32, 1536, 1024], P('fsdp')
- output 2: float32 [2, 1024, 4096], P(None, 'fsdp')
- output 3: float32 [2, 4096, 1024], P(None, 'fsdp')
- output 4: float32 [2, 1024, 4096], P(None, 'fsdp')
- output 5: float32 [2, 4096, 1024], P(None, 'fsdp')
- output 6: float32 [2, 1024, 4096], P(None, 'fsdp')
- output 7: float32 [2, 4096, 1024], P(None, 'fsdp')
All inputs are finite; a program needn't handle non-finite values.
Results may differ from the reference program's by a relative error of at most 0.00842076.
Values are sent between devices in bfloat16 or wider.
A program may use at most 1 GiB of HBM per device.

```python
import math
import jax
import jax.numpy as jnp
from jax import lax

LAYERS = 2
ADAM_STEP = 3
MICRO_STEPS = 2
GROUP_DEVS = 16
GLOBAL_BATCH = 32
SEQ_LEN = 1536
D_MODEL = 1024
D_FF = 4096

DEV_BATCH = GLOBAL_BATCH // GROUP_DEVS
LEARN_RATE = 0.001
BETA_ONE = 0.9
BETA_TWO = 0.95
ADAM_EPS = 1e-8
WEIGHT_DECAY = 0.1
CLIP_NORM = 0.1 * math.sqrt(2 * LAYERS * D_MODEL * D_FF)


def setup_inputs(seed: int = 0) -> dict:
    key_list = jax.random.split(jax.random.key(seed), 13)
    up_scale = D_MODEL ** -0.5
    down_scale = D_FF ** -0.5
    tok_shape = (GLOBAL_BATCH, SEQ_LEN, D_MODEL)
    up_shape = (LAYERS, D_MODEL, D_FF)
    down_shape = (LAYERS, D_FF, D_MODEL)
    master_up = jax.random.normal(key_list[3], up_shape, jnp.float32) * up_scale
    master_down = jax.random.normal(key_list[4], down_shape, jnp.float32) * down_scale
    w_up = master_up + 0.3 * up_scale * jax.random.normal(key_list[5], up_shape, jnp.float32)
    w_down = master_down + 0.3 * down_scale * jax.random.normal(key_list[6], down_shape, jnp.float32)
    grad_scale = (GLOBAL_BATCH * SEQ_LEN) ** -0.5
    return {
        "x_saved": jax.random.normal(key_list[0], (LAYERS,) + tok_shape, jnp.float32).astype(jnp.bfloat16),
        "grad_out": (grad_scale * jax.random.normal(key_list[1], tok_shape, jnp.float32)).astype(jnp.bfloat16),
        "x_next": jax.random.normal(key_list[2], tok_shape, jnp.float32).astype(jnp.bfloat16),
        "w_up": w_up.astype(jnp.bfloat16),
        "w_down": w_down.astype(jnp.bfloat16),
        "gacc_up": 0.3 * jax.random.normal(key_list[7], up_shape, jnp.float32),
        "gacc_down": 0.6 * jax.random.normal(key_list[8], down_shape, jnp.float32),
        "master_up": master_up,
        "master_down": master_down,
        "mom1_up": 0.01 * jax.random.normal(key_list[9], up_shape, jnp.float32),
        "mom1_down": 0.01 * jax.random.normal(key_list[10], down_shape, jnp.float32),
        "mom2_up": 0.0004 * (0.5 + jax.random.uniform(key_list[11], up_shape, jnp.float32)),
        "mom2_down": 0.0004 * (0.5 + jax.random.uniform(key_list[12], down_shape, jnp.float32)),
    }


def gelu_fn(pre_act):
    return jax.nn.gelu(pre_act, approximate=True)


def seq_backward(w_up, w_down, x_layers, grad_seq):
    grads_up = []
    grads_down = []
    grad_cur = grad_seq
    for layer_idx in range(LAYERS - 1, -1, -1):
        x_in = x_layers[layer_idx]
        pre_act = jnp.dot(x_in, w_up[layer_idx], preferred_element_type=jnp.float32)
        hidden_act, gelu_vjp = jax.vjp(gelu_fn, pre_act)
        d_act = jnp.dot(grad_cur, w_down[layer_idx].T, preferred_element_type=jnp.float32)
        d_pre = gelu_vjp(d_act)[0].astype(jnp.bfloat16)
        grads_down.append(jnp.dot(hidden_act.astype(jnp.bfloat16).T, grad_cur, preferred_element_type=jnp.float32))
        grads_up.append(jnp.dot(x_in.T, d_pre, preferred_element_type=jnp.float32))
        if layer_idx > 0:
            grad_cur = (grad_cur.astype(jnp.float32) + jnp.dot(d_pre, w_up[layer_idx].T, preferred_element_type=jnp.float32)).astype(jnp.bfloat16)
    return jnp.stack(grads_up[::-1]), jnp.stack(grads_down[::-1])


def device_partials(w_up, w_down, x_dev, grad_dev):
    def scan_body(acc_in, seq_idx):
        up_grad, down_grad = seq_backward(w_up, w_down, x_dev[:, seq_idx], grad_dev[seq_idx])
        return (acc_in[0] + up_grad, acc_in[1] + down_grad), None
    start_acc = (jnp.zeros((LAYERS, D_MODEL, D_FF), jnp.float32), jnp.zeros((LAYERS, D_FF, D_MODEL), jnp.float32))
    acc_pair, _ = lax.scan(scan_body, start_acc, jnp.arange(DEV_BATCH))
    return acc_pair[0].astype(jnp.bfloat16), acc_pair[1].astype(jnp.bfloat16)


def adamw_update(master_old, mom_one, mom_two, grad_clip):
    mom_one_new = BETA_ONE * mom_one + (1.0 - BETA_ONE) * grad_clip
    mom_two_new = BETA_TWO * mom_two + (1.0 - BETA_TWO) * grad_clip * grad_clip
    first_hat = mom_one_new / (1.0 - BETA_ONE ** ADAM_STEP)
    second_hat = mom_two_new / (1.0 - BETA_TWO ** ADAM_STEP)
    master_new = master_old - LEARN_RATE * (first_hat / (jnp.sqrt(second_hat) + ADAM_EPS) + WEIGHT_DECAY * master_old)
    return master_new, mom_one_new, mom_two_new


def seq_forward(w_up_new, w_down_new, x_seq):
    hidden_state = x_seq
    for layer_idx in range(LAYERS):
        pre_act = jnp.dot(hidden_state, w_up_new[layer_idx], preferred_element_type=jnp.float32)
        hidden_act = gelu_fn(pre_act).astype(jnp.bfloat16)
        hidden_state = (hidden_state.astype(jnp.float32) + jnp.dot(hidden_act, w_down_new[layer_idx], preferred_element_type=jnp.float32)).astype(jnp.bfloat16)
    return hidden_state


def reference(x_saved, grad_out, x_next, w_up, w_down, gacc_up, gacc_down, master_up, master_down, mom1_up, mom1_down, mom2_up, mom2_down):
    x_groups = x_saved.reshape(LAYERS, GROUP_DEVS, DEV_BATCH, SEQ_LEN, D_MODEL)
    grad_groups = grad_out.reshape(GROUP_DEVS, DEV_BATCH, SEQ_LEN, D_MODEL)

    def dev_body(acc_in, dev_idx):
        part_up, part_down = device_partials(w_up, w_down, x_groups[:, dev_idx], grad_groups[dev_idx])
        return (acc_in[0] + part_up.astype(jnp.float32), acc_in[1] + part_down.astype(jnp.float32)), None

    start_acc = (jnp.zeros((LAYERS, D_MODEL, D_FF), jnp.float32), jnp.zeros((LAYERS, D_FF, D_MODEL), jnp.float32))
    acc_pair, _ = lax.scan(dev_body, start_acc, jnp.arange(GROUP_DEVS))
    grad_up = (gacc_up + acc_pair[0]) / MICRO_STEPS
    grad_down = (gacc_down + acc_pair[1]) / MICRO_STEPS
    total_norm = jnp.sqrt(jnp.sum(grad_up * grad_up) + jnp.sum(grad_down * grad_down))
    clip_factor = jnp.minimum(1.0, CLIP_NORM / total_norm)
    new_up = adamw_update(master_up, mom1_up, mom2_up, grad_up * clip_factor)
    new_down = adamw_update(master_down, mom1_down, mom2_down, grad_down * clip_factor)
    w_up_new = new_up[0].astype(jnp.bfloat16)
    w_down_new = new_down[0].astype(jnp.bfloat16)
    x_out = lax.map(lambda x_seq: seq_forward(w_up_new, w_down_new, x_seq), x_next)
    return (x_out, new_up[0], new_down[0], new_up[1], new_down[1], new_up[2], new_down[2])
```

```python
import functools
import math
import jax
import jax.numpy as jnp
from jax import lax
from jax.experimental import pallas as pl
from jax.experimental.pallas import tpu as pltpu
from jax.sharding import PartitionSpec as P

LEARN_RATE = 0.001
BETA_ONE = 0.9
BETA_TWO = 0.95
ADAM_EPS = 1e-8
WEIGHT_DECAY = 0.1
ADAM_STEP = 3
MICRO_STEPS = 2

GELU_A = math.sqrt(2.0 / math.pi)
GELU_B = GELU_A * 0.044715
MESH = pl.DeviceIdType.MESH
STRIDES = (8, 4, 2, 1)
ORDERS = ((2, 1, 0), (1, 0, 2), (0, 2, 1))
TILE = 512


def gelu_fn(pre_act):
    return jax.nn.gelu(pre_act, approximate=True)


def adamw_update(master_old, mom_one, mom_two, grad_clip):
    mom_one_new = BETA_ONE * mom_one + (1.0 - BETA_ONE) * grad_clip
    mom_two_new = BETA_TWO * mom_two + (1.0 - BETA_TWO) * grad_clip * grad_clip
    first_hat = mom_one_new / (1.0 - BETA_ONE ** ADAM_STEP)
    second_hat = mom_two_new / (1.0 - BETA_TWO ** ADAM_STEP)
    master_new = master_old - LEARN_RATE * (first_hat / (jnp.sqrt(second_hat) + ADAM_EPS) + WEIGHT_DECAY * master_old)
    return master_new, mom_one_new, mom_two_new


def dot_nt(left, right):
    return lax.dot_general(left, right, (((1,), (1,)), ((), ())), preferred_element_type=jnp.float32)


def dot_tn(left, right):
    return lax.dot_general(left, right, (((0,), (0,)), ((), ())), preferred_element_type=jnp.float32)


def at_bits(picks, count):
    return tuple(picks.get(dim, slice(None)) for dim in range(count))


def backward_kernel(n_steps, n_chunks, cols, x_hbm, g_hbm, w1_ref, w2_ref, out1_ref, out2_ref, x_buf, g_buf, acc, act_buf, dh_buf, part1, part2, *rest):
    parts = (part1, part2)
    recv0, send1, keep1, recv1, send2, keep2, recv2, send3, keep3, recv3 = (rest[2 * i:2 * i + 2] for i in range(10))
    load_sem, send_sem0, recv_sem0, send_sem, recv_sem = rest[20:]
    outs = (out1_ref, out2_ref)
    step = pl.program_id(0)
    me = lax.axis_index("fsdp")
    bits = [lax.rem(me // stride, 2) for stride in STRIDES]
    peers = [me + (1 - 2 * bit) * stride for bit, stride in zip(bits, STRIDES)]
    tokens = x_buf.shape[0]
    sends = (send1, send2, send3)
    recvs = (recv1, recv2, recv3)

    def core_copy(mat, block):
        return pltpu.make_async_remote_copy(
            src_ref=parts[mat].at[:, :, :, 1 - bits[3]], dst_ref=recv0[mat].at[lax.rem(block, 2)],
            send_sem=send_sem0.at[mat], recv_sem=recv_sem0.at[mat, lax.rem(block, 2)],
            device_id=(peers[3],), device_id_type=MESH)

    def axis_copy(phase, mat, color, block):
        lo, hi = cols[mat][color]
        lead = (slice(None),) * (4 - phase)
        slot = (phase - 1) * 6 + mat * 3 + color
        return pltpu.make_async_remote_copy(
            src_ref=sends[phase - 1][mat].at[lead + (pl.ds(lo, hi - lo),)],
            dst_ref=recvs[phase - 1][mat].at[(lax.rem(block, 2),) + lead + (pl.ds(lo, hi - lo),)],
            send_sem=send_sem.at[slot], recv_sem=recv_sem.at[slot, lax.rem(block, 2)],
            device_id=(peers[ORDERS[color][phase - 1]],), device_id_type=MESH)

    def each_color():
        for mat in range(2):
            for color in range(3):
                yield mat, color, pl.ds(cols[mat][color][0], cols[mat][color][1] - cols[mat][color][0])

    @pl.when(step == 0)
    def _():
        barrier = pltpu.get_barrier_semaphore()
        for peer in peers:
            pl.semaphore_signal(barrier, inc=1, device_id=(peer,), device_id_type=MESH)
        load_x = pltpu.make_async_copy(x_hbm.at[1], x_buf, load_sem.at[0])
        load_g = pltpu.make_async_copy(g_hbm, g_buf, load_sem.at[1])
        load_x.start()
        load_g.start()
        acc[...] = jnp.zeros_like(acc)
        load_x.wait()
        load_g.wait()
        pl.semaphore_wait(barrier, 4)

    @pl.when(step == n_chunks)
    def _():
        load_x = pltpu.make_async_copy(x_hbm.at[0], x_buf, load_sem.at[0])
        load_x.start()
        load_x.wait()

    @pl.when(step < n_steps)
    def _():
        def tile_body(tile, carry):
            rows = pl.ds(pl.multiple_of(tile * TILE, TILE), TILE)
            pre = jnp.dot(x_buf[rows, :], w1_ref[...], preferred_element_type=jnp.float32)
            d_act = dot_nt(g_buf[rows, :], w2_ref[...].reshape(w1_ref.shape[1], w1_ref.shape[0]))
            square = pre * pre
            gate = 0.5 + 0.5 * jnp.tanh(pre * (GELU_A + GELU_B * square))
            act = pre * gate
            act_buf[rows, :] = act.astype(jnp.bfloat16)
            slope = gate + (act * (1.0 - gate)) * (2.0 * GELU_A + 6.0 * GELU_B * square)
            dh_buf[rows, :] = (d_act * slope).astype(jnp.bfloat16)
            return carry
        lax.fori_loop(0, tokens // TILE, tile_body, 0)

    @pl.when(step >= 4)
    def _():
        block = step - 4
        for mat, color, span in each_color():
            copy = axis_copy(3, mat, color, block)
            copy.wait_send()
            copy.wait_recv()
            outs[mat][:, span] = keep3[mat][:, span] + recv3[mat][lax.rem(block, 2), :, span]

    @pl.when((step >= 3) & (step < n_steps + 3))
    def _():
        block = step - 3
        for mat, color, span in each_color():
            copy = axis_copy(2, mat, color, block)
            copy.wait_send()
            copy.wait_recv()
            bit = bits[ORDERS[color][2]]
            slot = lax.rem(block, 2)
            send3[mat][:, span] = keep2[mat][1 - bit, :, span] + recv2[mat][slot, 1 - bit, :, span]
            keep3[mat][:, span] = keep2[mat][bit, :, span] + recv2[mat][slot, bit, :, span]
            axis_copy(3, mat, color, block).start()

    @pl.when((step >= 2) & (step < n_steps + 2))
    def _():
        block = step - 2
        for mat, color, span in each_color():
            copy = axis_copy(1, mat, color, block)
            copy.wait_send()
            copy.wait_recv()
            left = [axis for axis in range(3) if axis != ORDERS[color][0]]
            place = left.index(ORDERS[color][1])
            bit = bits[ORDERS[color][1]]
            slot = lax.rem(block, 2)
            for value, store in ((1 - bit, send2), (bit, keep2)):
                index = at_bits({place: value}, 2)
                store[mat][:, :, span] = keep1[mat][index + (slice(None), span)] + recv1[mat][(slot,) + index + (slice(None), span)]
            axis_copy(2, mat, color, block).start()

    @pl.when((step >= 1) & (step < n_steps + 1))
    def _():
        block = step - 1
        for mat in range(2):
            copy = core_copy(mat, block)
            copy.wait_send()
            copy.wait_recv()
        for mat, color, span in each_color():
            axis = ORDERS[color][0]
            slot = lax.rem(block, 2)
            for value, store in ((1 - bits[axis], send1), (bits[axis], keep1)):
                index = at_bits({axis: value}, 3)
                mine = parts[mat][index + (bits[3], slice(None), span)].astype(jnp.float32)
                store[mat][:, :, :, span] = mine + recv0[mat][(slot,) + index + (slice(None), span)].astype(jnp.float32)
            axis_copy(1, mat, color, block).start()

    @pl.when(step < n_steps)
    def _():
        part2[...] = dot_tn(act_buf[...], g_buf[...]).astype(jnp.bfloat16).reshape(part2.shape)
        core_copy(1, step).start()
        part1[...] = dot_tn(x_buf[...], dh_buf[...]).astype(jnp.bfloat16).reshape(part1.shape)
        core_copy(0, step).start()

    @pl.when(step < n_chunks)
    def _():
        def tile_body(tile, carry):
            rows = pl.ds(pl.multiple_of(tile * TILE, TILE), TILE)
            acc[rows, :] += dot_nt(dh_buf[rows, :], w1_ref[...])
            return carry
        lax.fori_loop(0, tokens // TILE, tile_body, 0)

    @pl.when(step == n_chunks - 1)
    def _():
        def tile_body(tile, carry):
            rows = pl.ds(pl.multiple_of(tile * TILE, TILE), TILE)
            g_buf[rows, :] = (g_buf[rows, :].astype(jnp.float32) + acc[rows, :]).astype(jnp.bfloat16)
            return carry
        lax.fori_loop(0, tokens // TILE, tile_body, 0)


def backward_sums(x_tokens, grad_tokens, w_up, w_down, n_dev):
    layers, model_width, ff_width = w_up.shape
    tokens = grad_tokens.shape[0]
    chunk = 512
    n_chunks = ff_width // chunk
    per_dev = chunk // n_dev
    rows_up = model_width // n_dev
    n_steps = layers * n_chunks
    cols = (((0, chunk // 4), (chunk // 4, chunk // 2), (chunk // 2, chunk)), ((0, 384), (384, 768), (768, model_width)))
    w1_view = w_up.reshape(layers, model_width, n_dev, n_chunks, per_dev).transpose(0, 3, 1, 2, 4).reshape(layers, n_chunks, model_width, chunk)
    w2_view = w_down.reshape(layers, n_dev, n_chunks, per_dev, model_width)

    def where(step):
        last = jnp.minimum(step, n_steps - 1)
        return layers - 1 - last // n_chunks, lax.rem(last, n_chunks)

    def pair(lead, dtype):
        return [pltpu.VMEM(lead + (rows_up, chunk), dtype), pltpu.VMEM(lead + (per_dev, model_width), dtype)]

    f32, b16 = jnp.float32, jnp.bfloat16
    scratch = [pltpu.VMEM((tokens, model_width), b16), pltpu.VMEM((tokens, model_width), b16), pltpu.VMEM((tokens, model_width), f32),
               pltpu.VMEM((tokens, chunk), b16), pltpu.VMEM((tokens, chunk), b16)]
    scratch += pair((2, 2, 2, 2), b16) + pair((2, 2, 2, 2), b16)
    for lead in ((2, 2), (2,), ()):
        scratch += pair(lead, f32) + pair(lead, f32) + pair((2,) + lead, f32)
    dma = pltpu.SemaphoreType.DMA
    scratch += [dma((2,)), dma((2,)), dma((2, 2)), dma((18,)), dma((18, 2))]
    hbm = pl.BlockSpec(memory_space=pl.ANY)
    out1, out2 = pl.pallas_call(
        functools.partial(backward_kernel, n_steps, n_chunks, cols),
        grid=(n_steps + 4,),
        in_specs=[hbm, hbm,
                  pl.BlockSpec((None, None, model_width, chunk), lambda s: (*where(s), 0, 0)),
                  pl.BlockSpec((None, n_dev, None, per_dev, model_width), lambda s: (where(s)[0], 0, where(s)[1], 0, 0))],
        out_specs=[pl.BlockSpec((None, rows_up, chunk), lambda s: (jnp.maximum(s - 4, 0), 0, 0)),
                   pl.BlockSpec((None, per_dev, model_width), lambda s: (jnp.maximum(s - 4, 0), 0, 0))],
        out_shape=[jax.ShapeDtypeStruct((n_steps, rows_up, chunk), f32), jax.ShapeDtypeStruct((n_steps, per_dev, model_width), f32)],
        scratch_shapes=scratch,
        compiler_params=pltpu.CompilerParams(vmem_limit_bytes=67_043_328, dimension_semantics=("arbitrary",), collective_id=0, has_side_effects=True),
        cost_estimate=pl.CostEstimate(flops=18 * tokens * model_width * ff_width, bytes_accessed=60_000_000, transcendentals=2 * tokens * ff_width),
        name="backward_reduce",
    )(x_tokens, grad_tokens, w1_view, w2_view)
    sums_up = out1.reshape(layers, n_chunks, rows_up, n_dev, per_dev)[::-1].transpose(0, 2, 3, 1, 4).reshape(layers, rows_up, ff_width)
    sums_down = out2.reshape(layers, n_chunks * per_dev, model_width)[::-1]
    return sums_up, sums_down


def solution(mesh):
    n_dev = mesh.shape["fsdp"]
    rows_spec = P(None, "fsdp")

    def local_step(x_saved, grad_out, x_next, w_up, w_down, gacc_up, gacc_down, master_up, master_down, mom1_up, mom1_down, mom2_up, mom2_down):
        layers, model_width, ff_width = w_up.shape
        clip_norm = 0.1 * math.sqrt(2 * layers * model_width * ff_width)
        sums_up, sums_down = backward_sums(x_saved.reshape(layers, -1, model_width), grad_out.reshape(-1, model_width), w_up, w_down, n_dev)
        grad_up = (gacc_up + sums_up) / MICRO_STEPS
        grad_down = (gacc_down + sums_down) / MICRO_STEPS
        local_sq = jnp.sum(grad_up * grad_up) + jnp.sum(grad_down * grad_down)
        clip_factor = jnp.minimum(1.0, clip_norm / jnp.sqrt(lax.psum(local_sq, "fsdp")))
        new_up = adamw_update(master_up, mom1_up, mom2_up, grad_up * clip_factor)
        new_down = adamw_update(master_down, mom1_down, mom2_down, grad_down * clip_factor)
        up_shard = new_up[0].astype(jnp.bfloat16)
        down_shard = new_down[0].astype(jnp.bfloat16)
        hidden_state = x_next.reshape(-1, x_next.shape[2])
        for layer_idx in range(layers):
            w_layer_up = lax.all_gather(up_shard[layer_idx], "fsdp", axis=0, tiled=True)
            w_layer_down = lax.all_gather(down_shard[layer_idx], "fsdp", axis=0, tiled=True)
            pre_act = jnp.dot(hidden_state, w_layer_up, preferred_element_type=jnp.float32)
            hidden_act = gelu_fn(pre_act).astype(jnp.bfloat16)
            hidden_state = (hidden_state.astype(jnp.float32) + jnp.dot(hidden_act, w_layer_down, preferred_element_type=jnp.float32)).astype(jnp.bfloat16)
        return (hidden_state.reshape(x_next.shape), new_up[0], new_down[0], new_up[1], new_down[1], new_up[2], new_down[2])

    return jax.shard_map(local_step, mesh=mesh, in_specs=(rows_spec, P("fsdp"), P("fsdp"), P(), P(), rows_spec, rows_spec, rows_spec, rows_spec, rows_spec, rows_spec, rows_spec, rows_spec), out_specs=(P("fsdp"), rows_spec, rows_spec, rows_spec, rows_spec, rows_spec, rows_spec), check_vma=False)
```

```python
import functools
import math
import jax
import jax.numpy as jnp
from jax import lax
from jax.experimental import pallas as pl
from jax.experimental.pallas import tpu as pltpu
from jax.sharding import PartitionSpec as P

LEARN_RATE = 0.001
BETA_ONE = 0.9
BETA_TWO = 0.95
ADAM_EPS = 1e-8
WEIGHT_DECAY = 0.1
ADAM_STEP = 3
MICRO_STEPS = 2

GELU_A = math.sqrt(2.0 / math.pi)
GELU_B = GELU_A * 0.044715
MESH = pl.DeviceIdType.MESH
STRIDES = (8, 4, 2, 1)
ORDERS = ((2, 1, 0), (1, 0, 2), (0, 2, 1))
TILE = 512
LANES = 128
ROWS = 128


def adamw_update(master_old, mom_one, mom_two, grad_clip):
    mom_one_new = BETA_ONE * mom_one + (1.0 - BETA_ONE) * grad_clip
    mom_two_new = BETA_TWO * mom_two + (1.0 - BETA_TWO) * grad_clip * grad_clip
    first_hat = mom_one_new / (1.0 - BETA_ONE ** ADAM_STEP)
    second_hat = mom_two_new / (1.0 - BETA_TWO ** ADAM_STEP)
    master_new = master_old - LEARN_RATE * (first_hat / (jnp.sqrt(second_hat) + ADAM_EPS) + WEIGHT_DECAY * master_old)
    return master_new, mom_one_new, mom_two_new


def dot_nt(left, right):
    return lax.dot_general(left, right, (((1,), (1,)), ((), ())), preferred_element_type=jnp.float32)


def dot_tn(left, right):
    return lax.dot_general(left, right, (((0,), (0,)), ((), ())), preferred_element_type=jnp.float32)


def at_bits(picks, count):
    return tuple(picks.get(dim, slice(None)) for dim in range(count))


def backward_kernel(n_steps, n_chunks, cols, x_hbm, g_hbm, w1_hbm, w2_ref, out1_ref, out2_ref, x_buf, g_buf, acc, act_buf, dh_buf, w1_group, w1_ref, part1, part2, *rest):
    parts = (part1, part2)
    recv0, send1, keep1, recv1, send2, keep2, recv2, send3, keep3, recv3 = (rest[2 * i:2 * i + 2] for i in range(10))
    load_sem, group_sem, send_sem0, recv_sem0, send_sem, recv_sem = rest[20:]
    step = pl.program_id(0)
    me = lax.axis_index("fsdp")
    bits = [lax.rem(me // stride, 2) for stride in STRIDES]
    peers = [me + (1 - 2 * bit) * stride for bit, stride in zip(bits, STRIDES)]
    tokens = x_buf.shape[0]
    sends = (send1, send2, send3)
    recvs = (recv1, recv2, recv3)

    def core_copy(mat, block):
        return pltpu.make_async_remote_copy(
            src_ref=parts[mat].at[:, :, :, 1 - bits[3]], dst_ref=recv0[mat].at[lax.rem(block, 2)],
            send_sem=send_sem0.at[mat], recv_sem=recv_sem0.at[mat, lax.rem(block, 2)],
            device_id=(peers[3],), device_id_type=MESH)

    def axis_copy(phase, mat, color, block):
        lo, hi = cols[mat][color]
        lead = (slice(None),) * (4 - phase)
        slot = (phase - 1) * 6 + mat * 3 + color
        return pltpu.make_async_remote_copy(
            src_ref=sends[phase - 1][mat].at[lead + (pl.ds(lo, hi - lo),)],
            dst_ref=recvs[phase - 1][mat].at[(lax.rem(block, 2),) + lead + (pl.ds(lo, hi - lo),)],
            send_sem=send_sem.at[slot], recv_sem=recv_sem.at[slot, lax.rem(block, 2)],
            device_id=(peers[ORDERS[color][phase - 1]],), device_id_type=MESH)

    def each_color():
        for mat in range(2):
            for color in range(3):
                yield mat, color, pl.ds(cols[mat][color][0], cols[mat][color][1] - cols[mat][color][0])

    n_dev, per_dev = w2_ref.shape[:2]
    spread = LANES // per_dev

    def lane_part():
        return lax.broadcasted_iota(jnp.int32, (ROWS, LANES), 1) // per_dev

    def group_copies(layer, half):
        return [pltpu.make_async_copy(
            w1_hbm.at[layer, :, pl.ds(pl.multiple_of((dev * n_chunks // spread + half) * LANES, LANES), LANES)],
            w1_group.at[dev], group_sem.at[dev]) for dev in range(n_dev)]

    @pl.when(step == 0)
    def _():
        for copy in group_copies(w1_hbm.shape[0] - 1, 0):
            copy.start()
        barrier = pltpu.get_barrier_semaphore()
        for peer in peers:
            pl.semaphore_signal(barrier, inc=1, device_id=(peer,), device_id_type=MESH)
        load_x = pltpu.make_async_copy(x_hbm.at[1], x_buf, load_sem.at[0])
        load_g = pltpu.make_async_copy(g_hbm, g_buf, load_sem.at[1])
        load_x.start()
        load_g.start()
        acc[...] = jnp.zeros_like(acc)
        load_x.wait()
        load_g.wait()
        pl.semaphore_wait(barrier, 4)

    @pl.when(step == n_chunks)
    def _():
        load_x = pltpu.make_async_copy(x_hbm.at[0], x_buf, load_sem.at[0])
        load_x.start()
        load_x.wait()

    @pl.when((step < n_steps) & (lax.rem(step, spread) == 0))
    def _():
        for copy in group_copies(0, 0):
            copy.wait()

    @pl.when(step < n_steps)
    def _():
        phase = lax.rem(step, spread)

        def row_body(block, carry):
            rows = pl.ds(pl.multiple_of(block * ROWS, ROWS), ROWS)
            part = lane_part()
            for tile in range(n_dev // spread):
                merged = None
                for place in range(spread):
                    moved = w1_group[tile * spread + place, rows, :].astype(jnp.float32)
                    moved = pltpu.roll(moved, lax.rem(place - phase + spread, spread) * per_dev, 1)
                    merged = moved if merged is None else jnp.where(part == place, moved, merged)
                w1_ref[rows, tile * LANES:(tile + 1) * LANES] = merged.astype(jnp.bfloat16)
            return carry
        lax.fori_loop(0, w1_ref.shape[0] // ROWS, row_body, 0)

    @pl.when((step < n_steps - 1) & (lax.rem(step, spread) == spread - 1))
    def _():
        following = step + 1
        for copy in group_copies(w1_hbm.shape[0] - 1 - following // n_chunks, lax.rem(following, n_chunks) // spread):
            copy.start()

    @pl.when(step < n_steps)
    def _():
        def tile_body(tile, carry):
            rows = pl.ds(pl.multiple_of(tile * TILE, TILE), TILE)
            pre = jnp.dot(x_buf[rows, :], w1_ref[...], preferred_element_type=jnp.float32)
            d_act = dot_nt(g_buf[rows, :], w2_ref[...].reshape(w1_ref.shape[1], w1_ref.shape[0]))
            square = pre * pre
            gate = 0.5 + 0.5 * jnp.tanh(pre * (GELU_A + GELU_B * square))
            act = pre * gate
            act_buf[rows, :] = act.astype(jnp.bfloat16)
            slope = gate + (act * (1.0 - gate)) * (2.0 * GELU_A + 6.0 * GELU_B * square)
            dh_buf[rows, :] = (d_act * slope).astype(jnp.bfloat16)
            return carry
        lax.fori_loop(0, tokens // TILE, tile_body, 0)

    @pl.when(step >= 4)
    def _():
        block = step - 4
        for mat, color, span in each_color():
            copy = axis_copy(3, mat, color, block)
            copy.wait_send()
            copy.wait_recv()
            total = keep3[mat][:, span] + recv3[mat][lax.rem(block, 2), :, span]
            if mat == 1:
                out2_ref[:, span] = total
            else:
                keep3[0][:, span] = total
        chunk = lax.rem(block, n_chunks)

        @pl.when(chunk == 0)
        def _():
            out1_ref[...] = jnp.zeros_like(out1_ref)
        phase = lax.rem(chunk, spread)
        part = lax.broadcasted_iota(jnp.int32, (out1_ref.shape[0], LANES), 1) // per_dev
        for dev in range(n_dev):
            tile = dev // spread
            moved = pltpu.roll(keep3[0][:, tile * LANES:(tile + 1) * LANES], lax.rem(phase - dev % spread + spread, spread) * per_dev, 1)
            spot = pl.ds(pl.multiple_of((dev * n_chunks // spread + chunk // spread) * LANES, LANES), LANES)
            out1_ref[:, spot] = jnp.where(part == phase, moved, out1_ref[:, spot])

    @pl.when((step >= 3) & (step < n_steps + 3))
    def _():
        block = step - 3
        for mat, color, span in each_color():
            copy = axis_copy(2, mat, color, block)
            copy.wait_send()
            copy.wait_recv()
            bit = bits[ORDERS[color][2]]
            slot = lax.rem(block, 2)
            send3[mat][:, span] = keep2[mat][1 - bit, :, span] + recv2[mat][slot, 1 - bit, :, span]
            keep3[mat][:, span] = keep2[mat][bit, :, span] + recv2[mat][slot, bit, :, span]
            axis_copy(3, mat, color, block).start()

    @pl.when((step >= 2) & (step < n_steps + 2))
    def _():
        block = step - 2
        for mat, color, span in each_color():
            copy = axis_copy(1, mat, color, block)
            copy.wait_send()
            copy.wait_recv()
            left = [axis for axis in range(3) if axis != ORDERS[color][0]]
            place = left.index(ORDERS[color][1])
            bit = bits[ORDERS[color][1]]
            slot = lax.rem(block, 2)
            for value, store in ((1 - bit, send2), (bit, keep2)):
                index = at_bits({place: value}, 2)
                store[mat][:, :, span] = keep1[mat][index + (slice(None), span)] + recv1[mat][(slot,) + index + (slice(None), span)]
            axis_copy(2, mat, color, block).start()

    @pl.when((step >= 1) & (step < n_steps + 1))
    def _():
        block = step - 1
        for mat in range(2):
            copy = core_copy(mat, block)
            copy.wait_send()
            copy.wait_recv()
        for mat, color, span in each_color():
            axis = ORDERS[color][0]
            slot = lax.rem(block, 2)
            for value, store in ((1 - bits[axis], send1), (bits[axis], keep1)):
                index = at_bits({axis: value}, 3)
                mine = parts[mat][index + (bits[3], slice(None), span)].astype(jnp.float32)
                store[mat][:, :, :, span] = mine + recv0[mat][(slot,) + index + (slice(None), span)].astype(jnp.float32)
            axis_copy(1, mat, color, block).start()

    @pl.when(step < n_steps)
    def _():
        part2[...] = dot_tn(act_buf[...], g_buf[...]).astype(jnp.bfloat16).reshape(part2.shape)
        core_copy(1, step).start()
        part1[...] = dot_tn(x_buf[...], dh_buf[...]).astype(jnp.bfloat16).reshape(part1.shape)
        core_copy(0, step).start()

    @pl.when(step < n_chunks)
    def _():
        def tile_body(tile, carry):
            rows = pl.ds(pl.multiple_of(tile * TILE, TILE), TILE)
            acc[rows, :] += dot_nt(dh_buf[rows, :], w1_ref[...])
            return carry
        lax.fori_loop(0, tokens // TILE, tile_body, 0)

    @pl.when(step == n_chunks - 1)
    def _():
        def tile_body(tile, carry):
            rows = pl.ds(pl.multiple_of(tile * TILE, TILE), TILE)
            g_buf[rows, :] = (g_buf[rows, :].astype(jnp.float32) + acc[rows, :]).astype(jnp.bfloat16)
            return carry
        lax.fori_loop(0, tokens // TILE, tile_body, 0)


def backward_sums(x_tokens, grad_tokens, w_up, w_down, n_dev):
    layers, model_width, ff_width = w_up.shape
    tokens = grad_tokens.shape[0]
    chunk = 512
    n_chunks = ff_width // chunk
    per_dev = chunk // n_dev
    rows_up = model_width // n_dev
    n_steps = layers * n_chunks
    cols = (((0, chunk // 4), (chunk // 4, chunk // 2), (chunk // 2, chunk)), ((0, 384), (384, 768), (768, model_width)))
    w2_view = w_down.reshape(layers, n_dev, n_chunks, per_dev, model_width)

    def where(step):
        last = jnp.minimum(step, n_steps - 1)
        return layers - 1 - last // n_chunks, lax.rem(last, n_chunks)

    def pair(lead, dtype):
        return [pltpu.VMEM(lead + (rows_up, chunk), dtype), pltpu.VMEM(lead + (per_dev, model_width), dtype)]

    f32, b16 = jnp.float32, jnp.bfloat16
    scratch = [pltpu.VMEM((tokens, model_width), b16), pltpu.VMEM((tokens, model_width), b16), pltpu.VMEM((tokens, model_width), f32),
               pltpu.VMEM((tokens, chunk), b16), pltpu.VMEM((tokens, chunk), b16),
               pltpu.VMEM((n_dev, model_width, LANES), b16), pltpu.VMEM((model_width, chunk), b16)]
    scratch += pair((2, 2, 2, 2), b16) + pair((2, 2, 2, 2), b16)
    for lead in ((2, 2), (2,), ()):
        scratch += pair(lead, f32) + pair(lead, f32) + pair((2,) + lead, f32)
    dma = pltpu.SemaphoreType.DMA
    scratch += [dma((2,)), dma((n_dev,)), dma((2,)), dma((2, 2)), dma((18,)), dma((18, 2))]
    hbm = pl.BlockSpec(memory_space=pl.ANY)
    out1, out2 = pl.pallas_call(
        functools.partial(backward_kernel, n_steps, n_chunks, cols),
        grid=(n_steps + 4,),
        in_specs=[hbm, hbm,
                  hbm,
                  pl.BlockSpec((None, n_dev, None, per_dev, model_width), lambda s: (where(s)[0], 0, where(s)[1], 0, 0))],
        out_specs=[pl.BlockSpec((None, rows_up, ff_width), lambda s: (where(jnp.maximum(s - 4, 0))[0], 0, 0)),
                   pl.BlockSpec((None, per_dev, model_width), lambda s: (*where(jnp.maximum(s - 4, 0)), 0))],
        out_shape=[jax.ShapeDtypeStruct((layers, rows_up, ff_width), f32), jax.ShapeDtypeStruct((layers, n_chunks * per_dev, model_width), f32)],
        scratch_shapes=scratch,
        compiler_params=pltpu.CompilerParams(vmem_limit_bytes=67_043_328, dimension_semantics=("arbitrary",), collective_id=0, has_side_effects=True),
        cost_estimate=pl.CostEstimate(flops=18 * tokens * model_width * ff_width, bytes_accessed=60_000_000, transcendentals=2 * tokens * ff_width),
        name="backward_reduce",
    )(x_tokens, grad_tokens, w_up, w2_view)
    return out1, out2


def norm_kernel(n_dev, value_ref, out_ref, gathered, send_sem, recv_sem):
    me = lax.axis_index("fsdp")
    barrier = pltpu.get_barrier_semaphore()
    for shift in range(1, n_dev):
        pl.semaphore_signal(barrier, inc=1, device_id=(lax.rem(me + shift, n_dev),), device_id_type=MESH)
    pl.semaphore_wait(barrier, n_dev - 1)

    def copy_of(shift, sender):
        return pltpu.make_async_remote_copy(
            src_ref=value_ref, dst_ref=gathered.at[sender], send_sem=send_sem.at[shift], recv_sem=recv_sem.at[sender],
            device_id=(lax.rem(me + shift, n_dev),), device_id_type=MESH)

    for shift in range(1, n_dev):
        copy_of(shift, me).start()
    gathered[me] = value_ref[...]
    for shift in range(1, n_dev):
        copy_of(shift, lax.rem(me + n_dev - shift, n_dev)).wait_recv()
    total = gathered[0]
    for dev in range(1, n_dev):
        total = total + gathered[dev]
    out_ref[...] = total
    for shift in range(1, n_dev):
        copy_of(shift, me).wait_send()


def global_sum(value, n_dev):
    tile = jnp.broadcast_to(value, (8, LANES))
    vmem = pl.BlockSpec(memory_space=pltpu.VMEM)
    dma = pltpu.SemaphoreType.DMA
    return pl.pallas_call(
        functools.partial(norm_kernel, n_dev), in_specs=[vmem], out_specs=vmem,
        out_shape=jax.ShapeDtypeStruct(tile.shape, jnp.float32),
        scratch_shapes=[pltpu.VMEM((n_dev,) + tile.shape, jnp.float32), dma((n_dev,)), dma((n_dev,))],
        compiler_params=pltpu.CompilerParams(collective_id=1, has_side_effects=True),
        name="norm_sum")(tile)[0, 0]


def forward_kernel(x_hbm, up0_hbm, down0_hbm, up1_hbm, down1_hbm, y_hbm, h_buf, act_buf, buf_a, buf_b, buf_c, load_sem, free_sem, send_sem, recv_sem):
    shards = (up0_hbm, down0_hbm, up1_hbm, down1_hbm)
    bufs = (buf_a, buf_b, buf_c, buf_a)
    me = lax.axis_index("fsdp")
    bits = [lax.rem(me // stride, 2) for stride in STRIDES]
    peers = [me + (1 - 2 * bit) * stride for bit, stride in zip(bits, STRIDES)]
    rows = up0_hbm.shape[0]
    tokens, width = h_buf.shape
    quarter = rows // 4
    pieces = ((0, 0, rows // 2), (0, rows // 2, rows), (1, 0, rows), (2, 0, rows), (3, 0, rows))
    n_tiles = tokens // TILE

    def spans(piece):
        _, lo, hi = pieces[piece]
        size = (hi - lo) // 16
        third = size // 3
        cuts = [0, third, 2 * third, size]
        if piece % 3 == 1:
            cuts = [0, third, size - third, size]
        if piece % 3 == 2:
            cuts = [0, size - 2 * third, size - third, size]
        return [(lo + 16 * cuts[color], 16 * (cuts[color + 1] - cuts[color])) for color in range(3)]

    def copies(piece, phase):
        matrix = pieces[piece][0]
        out = []
        for color, (lo, size) in enumerate(spans(piece)):
            order = ORDERS[color]
            picks = {axis: bits[axis] for axis in range(4)}
            for axis in order[:min(phase, 2)]:
                picks.pop(axis)
            if phase == 4:
                picks[order[2]] = 1 - bits[order[2]]
            where = at_bits(picks, 4) + (pl.ds(lo, size),)
            axis = order[phase] if phase < 3 else 3
            slot = (piece * 5 + phase) * 3 + color
            out.append(pltpu.make_async_remote_copy(
                src_ref=bufs[matrix].at[where], dst_ref=bufs[matrix].at[where],
                send_sem=send_sem.at[slot], recv_sem=recv_sem.at[slot],
                device_id=(peers[axis],), device_id_type=MESH))
        return out

    def start(piece, phase):
        for copy in copies(piece, phase):
            copy.start()

    def arrived(piece, phase):
        for copy in copies(piece, phase):
            copy.wait_recv()

    def second(piece):
        arrived(piece, 0)
        start(piece, 1)

    def third(piece):
        arrived(piece, 1)
        start(piece, 2)
        start(piece, 3)

    def hand_over(piece):
        arrived(piece, 2)
        start(piece, 4)

    def complete(piece):
        arrived(piece, 3)
        arrived(piece, 4)

    def load(matrix):
        return pltpu.make_async_copy(shards[matrix], bufs[matrix].at[tuple(bits)], load_sem.at[matrix])

    barrier = pltpu.get_barrier_semaphore()
    for peer in peers:
        pl.semaphore_signal(barrier, inc=1, device_id=(peer,), device_id_type=MESH)
    for matrix in range(3):
        load(matrix).start()
    load_x = pltpu.make_async_copy(x_hbm, h_buf, load_sem.at[4])
    load_x.start()
    load(0).wait()
    pl.semaphore_wait(barrier, 4)
    start(0, 0)
    start(1, 0)
    load(1).wait()
    load(2).wait()
    second(0)
    second(1)
    third(0)
    start(2, 0)
    hand_over(0)
    third(1)
    second(2)
    start(3, 0)
    load_x.wait()
    complete(0)

    def weights(matrix, block):
        return bufs[matrix][:, :, :, :, pl.ds(pl.multiple_of(block * quarter, quarter), quarter), :].reshape(4 * 4 * quarter, width)

    def run(count, matrix, body, events):
        def step(index, carry):
            for when, event in events.items():
                pl.when(index == when)(event)
            body(index, matrix)
            return carry
        lax.fori_loop(0, count, step, 0)

    def up(index, matrix):
        block, tile = index // n_tiles, lax.rem(index, n_tiles)
        span = pl.ds(pl.multiple_of(tile * TILE, TILE), TILE)
        pre = jnp.dot(h_buf[span, :], weights(matrix, block), preferred_element_type=jnp.float32)
        gate = 0.5 + 0.5 * jnp.tanh(pre * (GELU_A + GELU_B * (pre * pre)))
        act_buf[block, span, :] = (pre * gate).astype(jnp.bfloat16)

    def down(tile, matrix):
        span = pl.ds(pl.multiple_of(tile * TILE, TILE), TILE)
        total = h_buf[span, :].astype(jnp.float32)
        for block in range(4):
            total = total + jnp.dot(act_buf[block, span, :], bufs[matrix][block // 2, block % 2].reshape(width, width), preferred_element_type=jnp.float32)
        h_buf[span, :] = total.astype(jnp.bfloat16)

    def store(tile):
        span = pl.ds(pl.multiple_of(tile * TILE, TILE), TILE)
        return pltpu.make_async_copy(h_buf.at[span, :], y_hbm.at[span, :], load_sem.at[5 + tile])

    def down_last(tile, matrix):
        down(tile, matrix)
        store(tile).start()

    def event_second():
        hand_over(1)
        third(2)
        second(3)

    def event_third():
        hand_over(2)
        third(3)

    def event_fourth():
        hand_over(3)
        third(4)

    run(4 * n_tiles, 0, up, {2 * n_tiles - 1: event_second, 2 * n_tiles: lambda: complete(1), 4 * n_tiles - 1: event_third})
    for piece in (0, 1):
        for phase in range(5):
            for copy in copies(piece, phase):
                copy.wait_send()
    for peer in peers:
        pl.semaphore_signal(free_sem, inc=1, device_id=(peer,), device_id_type=MESH)
    load(3).start()
    complete(2)
    load(3).wait()
    pl.semaphore_wait(free_sem, 4)
    start(4, 0)
    run(n_tiles, 1, down, {2: lambda: second(4), n_tiles - 1: event_fourth})
    complete(3)
    run(4 * n_tiles, 2, up, {4 * n_tiles - 3: lambda: hand_over(4)})
    complete(4)
    run(n_tiles, 3, down_last, {})
    for piece in (2, 3, 4):
        for phase in range(5):
            for copy in copies(piece, phase):
                copy.wait_send()
    for tile in range(n_tiles):
        store(tile).wait()


def forward_stack(x_tokens, up_shard, down_shard, n_dev):
    tokens, model_width = x_tokens.shape
    layers, rows, ff_width = up_shard.shape
    blocks = ff_width // model_width
    up_blocks = up_shard.reshape(layers, rows, blocks, model_width).transpose(0, 2, 1, 3).reshape(layers, blocks * rows, model_width)
    hbm = pl.BlockSpec(memory_space=pl.ANY)
    b16 = jnp.bfloat16
    gathered = pltpu.VMEM((2, 2, 2, 2, blocks * rows, model_width), b16)
    dma = pltpu.SemaphoreType.DMA
    return pl.pallas_call(
        forward_kernel, in_specs=[hbm] * 5, out_specs=hbm,
        out_shape=jax.ShapeDtypeStruct((tokens, model_width), b16),
        scratch_shapes=[pltpu.VMEM((tokens, model_width), b16), pltpu.VMEM((blocks, tokens, model_width), b16), gathered, gathered, gathered,
                        dma((5 + tokens // TILE,)), pltpu.SemaphoreType.REGULAR, dma((75,)), dma((75,))],
        compiler_params=pltpu.CompilerParams(vmem_limit_bytes=67_043_328, collective_id=2, has_side_effects=True),
        cost_estimate=pl.CostEstimate(flops=8 * tokens * model_width * ff_width, bytes_accessed=20_000_000, transcendentals=2 * tokens * ff_width),
        name="gather_forward",
    )(x_tokens, up_blocks[0], down_shard[0], up_blocks[1], down_shard[1])


def solution(mesh):
    n_dev = mesh.shape["fsdp"]
    rows_spec = P(None, "fsdp")

    def local_step(x_saved, grad_out, x_next, w_up, w_down, gacc_up, gacc_down, master_up, master_down, mom1_up, mom1_down, mom2_up, mom2_down):
        layers, model_width, ff_width = w_up.shape
        clip_norm = 0.1 * math.sqrt(2 * layers * model_width * ff_width)
        sums_up, sums_down = backward_sums(x_saved.reshape(layers, -1, model_width), grad_out.reshape(-1, model_width), w_up, w_down, n_dev)
        grad_up = (gacc_up + sums_up) / MICRO_STEPS
        grad_down = (gacc_down + sums_down) / MICRO_STEPS
        local_sq = jnp.sum(grad_up * grad_up) + jnp.sum(grad_down * grad_down)
        clip_factor = jnp.minimum(1.0, clip_norm / jnp.sqrt(global_sum(local_sq, n_dev)))
        new_up = adamw_update(master_up, mom1_up, mom2_up, grad_up * clip_factor)
        new_down = adamw_update(master_down, mom1_down, mom2_down, grad_down * clip_factor)
        up_shard = new_up[0].astype(jnp.bfloat16)
        down_shard = new_down[0].astype(jnp.bfloat16)
        hidden_state = forward_stack(x_next.reshape(-1, model_width), up_shard, down_shard, n_dev)
        return (hidden_state.reshape(x_next.shape), new_up[0], new_down[0], new_up[1], new_down[1], new_up[2], new_down[2])

    return jax.shard_map(local_step, mesh=mesh, in_specs=(rows_spec, P("fsdp"), P("fsdp"), P(), P(), rows_spec, rows_spec, rows_spec, rows_spec, rows_spec, rows_spec, rows_spec, rows_spec), out_specs=(P("fsdp"), rows_spec, rows_spec, rows_spec, rows_spec, rows_spec, rows_spec), check_vma=False)
```

```python
import functools
import math
import jax
import jax.numpy as jnp
from jax import lax
from jax.experimental import pallas as pl
from jax.experimental.pallas import tpu as pltpu
from jax.sharding import PartitionSpec as P

LEARN_RATE = 0.001
BETA_ONE = 0.9
BETA_TWO = 0.95
ADAM_EPS = 1e-8
WEIGHT_DECAY = 0.1
ADAM_STEP = 3
MICRO_STEPS = 2

GELU_A = math.sqrt(2.0 / math.pi)
GELU_B = GELU_A * 0.044715
MESH = pl.DeviceIdType.MESH
STRIDES = (8, 4, 2, 1)
ORDERS = ((2, 1, 0), (1, 0, 2), (0, 2, 1))
TILE = 512
LANES = 128
ROWS = 128
TILE_B = 384


def adamw_update(master_old, mom_one, mom_two, grad_clip):
    mom_one_new = BETA_ONE * mom_one + (1.0 - BETA_ONE) * grad_clip
    mom_two_new = BETA_TWO * mom_two + (1.0 - BETA_TWO) * grad_clip * grad_clip
    first_hat = mom_one_new / (1.0 - BETA_ONE ** ADAM_STEP)
    second_hat = mom_two_new / (1.0 - BETA_TWO ** ADAM_STEP)
    master_new = master_old - LEARN_RATE * (first_hat / (jnp.sqrt(second_hat) + ADAM_EPS) + WEIGHT_DECAY * master_old)
    return master_new, mom_one_new, mom_two_new


def dot_nt(left, right):
    return lax.dot_general(left, right, (((1,), (1,)), ((), ())), preferred_element_type=jnp.float32)


def at_bits(picks, count):
    return tuple(picks.get(dim, slice(None)) for dim in range(count))


def backward_kernel(n_steps, n_chunks, cols, x_hbm, g_hbm, w1_hbm, w2_ref, out1_ref, out2_ref, x_buf, g_buf, x_turned, acc, act_turned, dh_buf, w1_group, w1_slots, part1, part2, *rest):
    parts = (part1, part2)
    recv0, send1, keep1, recv1, send2, keep2, recv2, send3, keep3, recv3 = (rest[2 * i:2 * i + 2] for i in range(10))
    load_sem, group_sem, send_sem0, recv_sem0, send_sem, recv_sem = rest[20:]
    step = pl.program_id(0)
    me = lax.axis_index("fsdp")
    bits = [lax.rem(me // stride, 2) for stride in STRIDES]
    peers = [me + (1 - 2 * bit) * stride for bit, stride in zip(bits, STRIDES)]
    tokens = x_buf.shape[0]
    sends = (send1, send2, send3)
    recvs = (recv1, recv2, recv3)

    def core_copy(mat, block):
        return pltpu.make_async_remote_copy(
            src_ref=parts[mat].at[:, :, :, 1 - bits[3]], dst_ref=recv0[mat].at[lax.rem(block, 2)],
            send_sem=send_sem0.at[mat], recv_sem=recv_sem0.at[mat, lax.rem(block, 2)],
            device_id=(peers[3],), device_id_type=MESH)

    def axis_copy(phase, mat, color, block):
        lo, hi = cols[mat][color]
        lead = (slice(None),) * (4 - phase)
        slot = (phase - 1) * 6 + mat * 3 + color
        return pltpu.make_async_remote_copy(
            src_ref=sends[phase - 1][mat].at[lead + (pl.ds(lo, hi - lo),)],
            dst_ref=recvs[phase - 1][mat].at[(lax.rem(block, 2),) + lead + (pl.ds(lo, hi - lo),)],
            send_sem=send_sem.at[slot], recv_sem=recv_sem.at[slot, lax.rem(block, 2)],
            device_id=(peers[ORDERS[color][phase - 1]],), device_id_type=MESH)

    def each_color():
        for mat in range(2):
            for color in range(3):
                yield mat, color, pl.ds(cols[mat][color][0], cols[mat][color][1] - cols[mat][color][0])

    n_dev, per_dev = w2_ref.shape[:2]
    spread = LANES // per_dev

    def lane_part():
        return lax.broadcasted_iota(jnp.int32, (ROWS, LANES), 1) // per_dev

    def group_copies(layer, half):
        return [pltpu.make_async_copy(
            w1_hbm.at[layer, :, pl.ds(pl.multiple_of((dev * n_chunks // spread + half) * LANES, LANES), LANES)],
            w1_group.at[dev], group_sem.at[dev]) for dev in range(n_dev)]

    @pl.when(step == 0)
    def _():
        for copy in group_copies(w1_hbm.shape[0] - 1, 0):
            copy.start()
        barrier = pltpu.get_barrier_semaphore()
        for peer in peers:
            pl.semaphore_signal(barrier, inc=1, device_id=(peer,), device_id_type=MESH)
        load_x = pltpu.make_async_copy(x_hbm.at[1], x_buf, load_sem.at[0])
        load_g = pltpu.make_async_copy(g_hbm, g_buf, load_sem.at[1])
        load_x.start()
        load_g.start()
        acc[...] = jnp.zeros_like(acc)
        load_x.wait()
        load_g.wait()
        pl.semaphore_wait(barrier, 4)

    @pl.when(step == n_chunks)
    def _():
        load_x = pltpu.make_async_copy(x_hbm.at[0], x_buf, load_sem.at[0])
        load_x.start()
        load_x.wait()

    w1_ref = w1_slots.at[lax.rem(step, 2)]

    def order_columns(rows, phase, target):
        part = lane_part()
        for tile in range(n_dev // spread):
            merged = None
            for place in range(spread):
                moved = w1_group[tile * spread + place, rows, :].astype(jnp.float32)
                moved = pltpu.roll(moved, lax.rem(place - phase + spread, spread) * per_dev, 1)
                merged = moved if merged is None else jnp.where(part == place, moved, merged)
            target[rows, tile * LANES:(tile + 1) * LANES] = merged.astype(jnp.bfloat16)

    @pl.when(step == 0)
    def _():
        for copy in group_copies(0, 0):
            copy.wait()

        def row_body(block, carry):
            order_columns(pl.ds(pl.multiple_of(block * ROWS, ROWS), ROWS), 0, w1_slots.at[0])
            return carry
        lax.fori_loop(0, x_buf.shape[1] // ROWS, row_body, 0)

    @pl.when((step < n_steps - 1) & (lax.rem(step, spread) == spread - 1))
    def _():
        for copy in group_copies(0, 0):
            copy.wait()

    def tile_body(tile, turn_x):
        rows = pl.ds(pl.multiple_of(tile * TILE_B, TILE_B), TILE_B)
        pre = jnp.dot(x_buf[rows, :], w1_ref[...], preferred_element_type=jnp.float32)
        d_act = dot_nt(g_buf[rows, :], w2_ref[...].reshape(w1_ref.shape[1], w1_ref.shape[0]))
        square = pre * pre
        gate = 0.5 + 0.5 * jnp.tanh(pre * (GELU_A + GELU_B * square))
        act = pre * gate
        act_turned[:, rows] = act.astype(jnp.bfloat16).T
        slope = gate + (act * (1.0 - gate)) * (2.0 * GELU_A + 6.0 * GELU_B * square)
        dh_buf[rows, :] = (d_act * slope).astype(jnp.bfloat16)
        order_columns(pl.ds(pl.multiple_of(tile * ROWS, ROWS), ROWS), lax.rem(step + 1, spread), w1_slots.at[lax.rem(step + 1, 2)])
        if turn_x:
            x_turned[:, rows] = x_buf[rows, :].T

    first = lax.rem(step, n_chunks) == 0

    @pl.when((step < n_steps) & first)
    def _():
        lax.fori_loop(0, tokens // TILE_B, lambda tile, carry: (tile_body(tile, True), carry)[1], 0)

    @pl.when((step < n_steps) & (lax.rem(step, n_chunks) > 0))
    def _():
        lax.fori_loop(0, tokens // TILE_B, lambda tile, carry: (tile_body(tile, False), carry)[1], 0)

    @pl.when((step < n_steps - 2) & (lax.rem(step, spread) == spread - 2))
    def _():
        following = step + 2
        for copy in group_copies(w1_hbm.shape[0] - 1 - following // n_chunks, lax.rem(following, n_chunks) // spread):
            copy.start()

    @pl.when(step >= 4)
    def _():
        block = step - 4
        for mat, color, span in each_color():
            copy = axis_copy(3, mat, color, block)
            copy.wait_send()
            copy.wait_recv()
            total = keep3[mat][:, span] + recv3[mat][lax.rem(block, 2), :, span]
            if mat == 1:
                out2_ref[:, span] = total
            else:
                keep3[0][:, span] = total
        chunk = lax.rem(block, n_chunks)

        @pl.when(chunk == 0)
        def _():
            out1_ref[...] = jnp.zeros_like(out1_ref)
        phase = lax.rem(chunk, spread)
        part = lax.broadcasted_iota(jnp.int32, (out1_ref.shape[0], LANES), 1) // per_dev
        for dev in range(n_dev):
            tile = dev // spread
            moved = pltpu.roll(keep3[0][:, tile * LANES:(tile + 1) * LANES], lax.rem(phase - dev % spread + spread, spread) * per_dev, 1)
            spot = pl.ds(pl.multiple_of((dev * n_chunks // spread + chunk // spread) * LANES, LANES), LANES)
            out1_ref[:, spot] = jnp.where(part == phase, moved, out1_ref[:, spot])

    @pl.when((step >= 3) & (step < n_steps + 3))
    def _():
        block = step - 3
        for mat, color, span in each_color():
            copy = axis_copy(2, mat, color, block)
            copy.wait_send()
            copy.wait_recv()
            bit = bits[ORDERS[color][2]]
            slot = lax.rem(block, 2)
            send3[mat][:, span] = keep2[mat][1 - bit, :, span] + recv2[mat][slot, 1 - bit, :, span]
            keep3[mat][:, span] = keep2[mat][bit, :, span] + recv2[mat][slot, bit, :, span]
            axis_copy(3, mat, color, block).start()

    @pl.when((step >= 2) & (step < n_steps + 2))
    def _():
        block = step - 2
        for mat, color, span in each_color():
            copy = axis_copy(1, mat, color, block)
            copy.wait_send()
            copy.wait_recv()
            left = [axis for axis in range(3) if axis != ORDERS[color][0]]
            place = left.index(ORDERS[color][1])
            bit = bits[ORDERS[color][1]]
            slot = lax.rem(block, 2)
            for value, store in ((1 - bit, send2), (bit, keep2)):
                index = at_bits({place: value}, 2)
                store[mat][:, :, span] = keep1[mat][index + (slice(None), span)] + recv1[mat][(slot,) + index + (slice(None), span)]
            axis_copy(2, mat, color, block).start()

    @pl.when((step >= 1) & (step < n_steps + 1))
    def _():
        block = step - 1
        for mat in range(2):
            copy = core_copy(mat, block)
            copy.wait_send()
            copy.wait_recv()
        for mat, color, span in each_color():
            axis = ORDERS[color][0]
            slot = lax.rem(block, 2)
            for value, store in ((1 - bits[axis], send1), (bits[axis], keep1)):
                index = at_bits({axis: value}, 3)
                mine = parts[mat][index + (bits[3], slice(None), span)].astype(jnp.float32)
                store[mat][:, :, :, span] = mine + recv0[mat][(slot,) + index + (slice(None), span)].astype(jnp.float32)
            axis_copy(1, mat, color, block).start()

    @pl.when(step < n_steps)
    def _():
        part2[...] = jnp.dot(act_turned[...], g_buf[...], preferred_element_type=jnp.float32).astype(jnp.bfloat16).reshape(part2.shape)
        core_copy(1, step).start()
        part1[...] = jnp.dot(x_turned[...], dh_buf[...], preferred_element_type=jnp.float32).astype(jnp.bfloat16).reshape(part1.shape)
        core_copy(0, step).start()

    @pl.when(step < n_chunks)
    def _():
        def tile_body(tile, carry):
            rows = pl.ds(pl.multiple_of(tile * TILE, TILE), TILE)
            acc[rows, :] += dot_nt(dh_buf[rows, :], w1_ref[...])
            return carry
        lax.fori_loop(0, tokens // TILE, tile_body, 0)

    @pl.when(step == n_chunks - 1)
    def _():
        def tile_body(tile, carry):
            rows = pl.ds(pl.multiple_of(tile * TILE, TILE), TILE)
            g_buf[rows, :] = (g_buf[rows, :].astype(jnp.float32) + acc[rows, :]).astype(jnp.bfloat16)
            return carry
        lax.fori_loop(0, tokens // TILE, tile_body, 0)


def backward_sums(x_tokens, grad_tokens, w_up, w_down, n_dev):
    layers, model_width, ff_width = w_up.shape
    tokens = grad_tokens.shape[0]
    chunk = 512
    n_chunks = ff_width // chunk
    per_dev = chunk // n_dev
    rows_up = model_width // n_dev
    n_steps = layers * n_chunks
    cols = (((0, chunk // 4), (chunk // 4, chunk // 2), (chunk // 2, chunk)), ((0, 384), (384, 768), (768, model_width)))
    w2_view = w_down.reshape(layers, n_dev, n_chunks, per_dev, model_width)

    def where(step):
        last = jnp.minimum(step, n_steps - 1)
        return layers - 1 - last // n_chunks, lax.rem(last, n_chunks)

    def pair(lead, dtype):
        return [pltpu.VMEM(lead + (rows_up, chunk), dtype), pltpu.VMEM(lead + (per_dev, model_width), dtype)]

    f32, b16 = jnp.float32, jnp.bfloat16
    scratch = [pltpu.VMEM((tokens, model_width), b16), pltpu.VMEM((tokens, model_width), b16), pltpu.VMEM((model_width, tokens), b16),
               pltpu.VMEM((tokens, model_width), f32), pltpu.VMEM((chunk, tokens), b16), pltpu.VMEM((tokens, chunk), b16),
               pltpu.VMEM((n_dev, model_width, LANES), b16), pltpu.VMEM((2, model_width, chunk), b16)]
    scratch += pair((2, 2, 2, 2), b16) + pair((2, 2, 2, 2), b16)
    for lead in ((2, 2), (2,), ()):
        scratch += pair(lead, f32) + pair(lead, f32) + pair((2,) + lead, f32)
    dma = pltpu.SemaphoreType.DMA
    scratch += [dma((2,)), dma((n_dev,)), dma((2,)), dma((2, 2)), dma((18,)), dma((18, 2))]
    hbm = pl.BlockSpec(memory_space=pl.ANY)
    out1, out2 = pl.pallas_call(
        functools.partial(backward_kernel, n_steps, n_chunks, cols),
        grid=(n_steps + 4,),
        in_specs=[hbm, hbm,
                  hbm,
                  pl.BlockSpec((None, n_dev, None, per_dev, model_width), lambda s: (where(s)[0], 0, where(s)[1], 0, 0))],
        out_specs=[pl.BlockSpec((None, rows_up, ff_width), lambda s: (where(jnp.maximum(s - 4, 0))[0], 0, 0)),
                   pl.BlockSpec((None, per_dev, model_width), lambda s: (*where(jnp.maximum(s - 4, 0)), 0))],
        out_shape=[jax.ShapeDtypeStruct((layers, rows_up, ff_width), f32), jax.ShapeDtypeStruct((layers, n_chunks * per_dev, model_width), f32)],
        scratch_shapes=scratch,
        compiler_params=pltpu.CompilerParams(vmem_limit_bytes=67_043_328, dimension_semantics=("arbitrary",), collective_id=0, has_side_effects=True),
        cost_estimate=pl.CostEstimate(flops=18 * tokens * model_width * ff_width, bytes_accessed=60_000_000, transcendentals=2 * tokens * ff_width),
        name="backward_reduce",
    )(x_tokens, grad_tokens, w_up, w2_view)
    return out1, out2


def norm_kernel(n_dev, value_ref, out_ref, gathered, send_sem, recv_sem):
    me = lax.axis_index("fsdp")
    barrier = pltpu.get_barrier_semaphore()
    for shift in range(1, n_dev):
        pl.semaphore_signal(barrier, inc=1, device_id=(lax.rem(me + shift, n_dev),), device_id_type=MESH)
    pl.semaphore_wait(barrier, n_dev - 1)

    def copy_of(shift, sender):
        return pltpu.make_async_remote_copy(
            src_ref=value_ref, dst_ref=gathered.at[sender], send_sem=send_sem.at[shift], recv_sem=recv_sem.at[sender],
            device_id=(lax.rem(me + shift, n_dev),), device_id_type=MESH)

    for shift in range(1, n_dev):
        copy_of(shift, me).start()
    gathered[me] = value_ref[...]
    for shift in range(1, n_dev):
        copy_of(shift, lax.rem(me + n_dev - shift, n_dev)).wait_recv()
    total = gathered[0]
    for dev in range(1, n_dev):
        total = total + gathered[dev]
    out_ref[...] = total
    for shift in range(1, n_dev):
        copy_of(shift, me).wait_send()


def global_sum(value, n_dev):
    tile = jnp.broadcast_to(value, (8, LANES))
    vmem = pl.BlockSpec(memory_space=pltpu.VMEM)
    dma = pltpu.SemaphoreType.DMA
    return pl.pallas_call(
        functools.partial(norm_kernel, n_dev), in_specs=[vmem], out_specs=vmem,
        out_shape=jax.ShapeDtypeStruct(tile.shape, jnp.float32),
        scratch_shapes=[pltpu.VMEM((n_dev,) + tile.shape, jnp.float32), dma((n_dev,)), dma((n_dev,))],
        compiler_params=pltpu.CompilerParams(collective_id=1, has_side_effects=True),
        name="norm_sum")(tile)[0, 0]


def forward_kernel(x_hbm, up0_hbm, down0_hbm, up1_hbm, down1_hbm, y_hbm, h_buf, act_buf, buf_a, buf_b, buf_c, load_sem, free_sem, send_sem, recv_sem):
    shards = (up0_hbm, down0_hbm, up1_hbm, down1_hbm)
    bufs = (buf_a, buf_b, buf_c, buf_a)
    me = lax.axis_index("fsdp")
    bits = [lax.rem(me // stride, 2) for stride in STRIDES]
    peers = [me + (1 - 2 * bit) * stride for bit, stride in zip(bits, STRIDES)]
    rows = up0_hbm.shape[0]
    tokens, width = h_buf.shape
    quarter = rows // 4
    pieces = ((0, 0, rows // 2), (0, rows // 2, rows), (1, 0, rows), (2, 0, rows), (3, 0, rows))
    n_tiles = tokens // TILE

    def spans(piece):
        _, lo, hi = pieces[piece]
        size = (hi - lo) // 16
        third = size // 3
        cuts = [0, third, 2 * third, size]
        if piece % 3 == 1:
            cuts = [0, third, size - third, size]
        if piece % 3 == 2:
            cuts = [0, size - 2 * third, size - third, size]
        return [(lo + 16 * cuts[color], 16 * (cuts[color + 1] - cuts[color])) for color in range(3)]

    def copies(piece, phase):
        matrix = pieces[piece][0]
        out = []
        for color, (lo, size) in enumerate(spans(piece)):
            order = ORDERS[color]
            picks = {axis: bits[axis] for axis in range(4)}
            for axis in order[:min(phase, 2)]:
                picks.pop(axis)
            if phase == 4:
                picks[order[2]] = 1 - bits[order[2]]
            where = at_bits(picks, 4) + (pl.ds(lo, size),)
            axis = order[phase] if phase < 3 else 3
            slot = (piece * 5 + phase) * 3 + color
            out.append(pltpu.make_async_remote_copy(
                src_ref=bufs[matrix].at[where], dst_ref=bufs[matrix].at[where],
                send_sem=send_sem.at[slot], recv_sem=recv_sem.at[slot],
                device_id=(peers[axis],), device_id_type=MESH))
        return out

    def start(piece, phase):
        for copy in copies(piece, phase):
            copy.start()

    def arrived(piece, phase):
        for copy in copies(piece, phase):
            copy.wait_recv()

    def second(piece):
        arrived(piece, 0)
        start(piece, 1)

    def third(piece):
        arrived(piece, 1)
        start(piece, 2)
        start(piece, 3)

    def hand_over(piece):
        arrived(piece, 2)
        start(piece, 4)

    def complete(piece):
        arrived(piece, 3)
        arrived(piece, 4)

    def load(matrix):
        return pltpu.make_async_copy(shards[matrix], bufs[matrix].at[tuple(bits)], load_sem.at[matrix])

    barrier = pltpu.get_barrier_semaphore()
    for peer in peers:
        pl.semaphore_signal(barrier, inc=1, device_id=(peer,), device_id_type=MESH)
    for matrix in range(3):
        load(matrix).start()
    load_x = pltpu.make_async_copy(x_hbm, h_buf, load_sem.at[4])
    load_x.start()
    load(0).wait()
    pl.semaphore_wait(barrier, 4)
    start(0, 0)
    start(1, 0)
    load(1).wait()
    load(2).wait()
    second(0)
    second(1)
    third(0)
    start(2, 0)
    hand_over(0)
    third(1)
    second(2)
    start(3, 0)
    load_x.wait()
    complete(0)

    def weights(matrix, block):
        return bufs[matrix][:, :, :, :, pl.ds(pl.multiple_of(block * quarter, quarter), quarter), :].reshape(4 * 4 * quarter, width)

    def run(count, matrix, body, events):
        def step(index, carry):
            for when, event in events.items():
                pl.when(index == when)(event)
            body(index, matrix)
            return carry
        lax.fori_loop(0, count, step, 0)

    def up(index, matrix):
        block, tile = index // n_tiles, lax.rem(index, n_tiles)
        span = pl.ds(pl.multiple_of(tile * TILE, TILE), TILE)
        pre = jnp.dot(h_buf[span, :], weights(matrix, block), preferred_element_type=jnp.float32)
        gate = 0.5 + 0.5 * jnp.tanh(pre * (GELU_A + GELU_B * (pre * pre)))
        act_buf[block, span, :] = (pre * gate).astype(jnp.bfloat16)

    def down(tile, matrix):
        span = pl.ds(pl.multiple_of(tile * TILE, TILE), TILE)
        total = h_buf[span, :].astype(jnp.float32)
        for block in range(4):
            total = total + jnp.dot(act_buf[block, span, :], bufs[matrix][block // 2, block % 2].reshape(width, width), preferred_element_type=jnp.float32)
        h_buf[span, :] = total.astype(jnp.bfloat16)

    def store(tile):
        span = pl.ds(pl.multiple_of(tile * TILE, TILE), TILE)
        return pltpu.make_async_copy(h_buf.at[span, :], y_hbm.at[span, :], load_sem.at[5 + tile])

    def down_last(tile, matrix):
        down(tile, matrix)
        store(tile).start()

    def event_second():
        hand_over(1)
        third(2)
        second(3)

    def event_third():
        hand_over(2)
        third(3)

    def event_fourth():
        hand_over(3)
        third(4)

    run(4 * n_tiles, 0, up, {2 * n_tiles - 1: event_second, 2 * n_tiles: lambda: complete(1), 4 * n_tiles - 1: event_third})
    for piece in (0, 1):
        for phase in range(5):
            for copy in copies(piece, phase):
                copy.wait_send()
    for peer in peers:
        pl.semaphore_signal(free_sem, inc=1, device_id=(peer,), device_id_type=MESH)
    load(3).start()
    complete(2)
    load(3).wait()
    pl.semaphore_wait(free_sem, 4)
    start(4, 0)
    run(n_tiles, 1, down, {2: lambda: second(4), n_tiles - 1: event_fourth})
    complete(3)
    run(4 * n_tiles, 2, up, {4 * n_tiles - 3: lambda: hand_over(4)})
    complete(4)
    run(n_tiles, 3, down_last, {})
    for piece in (2, 3, 4):
        for phase in range(5):
            for copy in copies(piece, phase):
                copy.wait_send()
    for tile in range(n_tiles):
        store(tile).wait()


def forward_stack(x_tokens, up_shard, down_shard, n_dev):
    tokens, model_width = x_tokens.shape
    layers, rows, ff_width = up_shard.shape
    blocks = ff_width // model_width
    up_blocks = up_shard.reshape(layers, rows, blocks, model_width).transpose(0, 2, 1, 3).reshape(layers, blocks * rows, model_width)
    hbm = pl.BlockSpec(memory_space=pl.ANY)
    b16 = jnp.bfloat16
    gathered = pltpu.VMEM((2, 2, 2, 2, blocks * rows, model_width), b16)
    dma = pltpu.SemaphoreType.DMA
    return pl.pallas_call(
        forward_kernel, in_specs=[hbm] * 5, out_specs=hbm,
        out_shape=jax.ShapeDtypeStruct((tokens, model_width), b16),
        scratch_shapes=[pltpu.VMEM((tokens, model_width), b16), pltpu.VMEM((blocks, tokens, model_width), b16), gathered, gathered, gathered,
                        dma((5 + tokens // TILE,)), pltpu.SemaphoreType.REGULAR, dma((75,)), dma((75,))],
        compiler_params=pltpu.CompilerParams(vmem_limit_bytes=67_043_328, collective_id=2, has_side_effects=True),
        cost_estimate=pl.CostEstimate(flops=8 * tokens * model_width * ff_width, bytes_accessed=20_000_000, transcendentals=2 * tokens * ff_width),
        name="gather_forward",
    )(x_tokens, up_blocks[0], down_shard[0], up_blocks[1], down_shard[1])


def solution(mesh):
    n_dev = mesh.shape["fsdp"]
    rows_spec = P(None, "fsdp")

    def local_step(x_saved, grad_out, x_next, w_up, w_down, gacc_up, gacc_down, master_up, master_down, mom1_up, mom1_down, mom2_up, mom2_down):
        layers, model_width, ff_width = w_up.shape
        clip_norm = 0.1 * math.sqrt(2 * layers * model_width * ff_width)
        sums_up, sums_down = backward_sums(x_saved.reshape(layers, -1, model_width), grad_out.reshape(-1, model_width), w_up, w_down, n_dev)
        grad_up = (gacc_up + sums_up) / MICRO_STEPS
        grad_down = (gacc_down + sums_down) / MICRO_STEPS
        local_sq = jnp.sum(grad_up * grad_up) + jnp.sum(grad_down * grad_down)
        clip_factor = jnp.minimum(1.0, clip_norm / jnp.sqrt(global_sum(local_sq, n_dev)))
        new_up = adamw_update(master_up, mom1_up, mom2_up, grad_up * clip_factor)
        new_down = adamw_update(master_down, mom1_down, mom2_down, grad_down * clip_factor)
        up_shard = new_up[0].astype(jnp.bfloat16)
        down_shard = new_down[0].astype(jnp.bfloat16)
        hidden_state = forward_stack(x_next.reshape(-1, model_width), up_shard, down_shard, n_dev)
        return (hidden_state.reshape(x_next.shape), new_up[0], new_down[0], new_up[1], new_down[1], new_up[2], new_down[2])

    return jax.shard_map(local_step, mesh=mesh, in_specs=(rows_spec, P("fsdp"), P("fsdp"), P(), P(), rows_spec, rows_spec, rows_spec, rows_spec, rows_spec, rows_spec, rows_spec, rows_spec), out_specs=(P("fsdp"), rows_spec, rows_spec, rows_spec, rows_spec, rows_spec, rows_spec), check_vma=False)
```

```python
import functools
import math
import jax
import jax.numpy as jnp
from jax import lax
from jax.experimental import pallas as pl
from jax.experimental.pallas import tpu as pltpu
from jax.sharding import PartitionSpec as P

LEARN_RATE = 0.001
BETA_ONE = 0.9
BETA_TWO = 0.95
ADAM_EPS = 1e-8
WEIGHT_DECAY = 0.1
ADAM_STEP = 3
MICRO_STEPS = 2

GELU_A = math.sqrt(2.0 / math.pi)
GELU_B = GELU_A * 0.044715
MESH = pl.DeviceIdType.MESH
STRIDES = (8, 4, 2, 1)
ORDERS = ((2, 1, 0), (1, 0, 2), (0, 2, 1))
TILE = 512
LANES = 128
ROWS = 128
TILE_B = 512


def adamw_update(master_old, mom_one, mom_two, grad_clip):
    mom_one_new = BETA_ONE * mom_one + (1.0 - BETA_ONE) * grad_clip
    mom_two_new = BETA_TWO * mom_two + (1.0 - BETA_TWO) * grad_clip * grad_clip
    first_hat = mom_one_new / (1.0 - BETA_ONE ** ADAM_STEP)
    second_hat = mom_two_new / (1.0 - BETA_TWO ** ADAM_STEP)
    master_new = master_old - LEARN_RATE * (first_hat / (jnp.sqrt(second_hat) + ADAM_EPS) + WEIGHT_DECAY * master_old)
    return master_new, mom_one_new, mom_two_new


def dot_nt(left, right):
    return lax.dot_general(left, right, (((1,), (1,)), ((), ())), preferred_element_type=jnp.float32)


def at_bits(picks, count):
    return tuple(picks.get(dim, slice(None)) for dim in range(count))


def backward_kernel(n_steps, n_chunks, cols, x_hbm, g_hbm, w1_hbm, w2_ref, out1_ref, out2_ref, x_buf, g_buf, x_turned, acc, act_turned, dh_buf, w1_group, w1_ref, w1_next, part1, part2, *rest):
    parts = (part1, part2)
    recv0, send1, keep1, recv1, send2, keep2, recv2, send3, keep3, recv3 = (rest[2 * i:2 * i + 2] for i in range(10))
    load_sem, group_sem, send_sem0, recv_sem0, send_sem, recv_sem = rest[20:]
    step = pl.program_id(0)
    me = lax.axis_index("fsdp")
    bits = [lax.rem(me // stride, 2) for stride in STRIDES]
    peers = [me + (1 - 2 * bit) * stride for bit, stride in zip(bits, STRIDES)]
    tokens = x_buf.shape[0]
    sends = (send1, send2, send3)
    recvs = (recv1, recv2, recv3)

    def core_copy(mat, block):
        return pltpu.make_async_remote_copy(
            src_ref=parts[mat].at[:, :, :, 1 - bits[3]], dst_ref=recv0[mat].at[lax.rem(block, 2)],
            send_sem=send_sem0.at[mat], recv_sem=recv_sem0.at[mat, lax.rem(block, 2)],
            device_id=(peers[3],), device_id_type=MESH)

    def axis_copy(phase, mat, color, block):
        lo, hi = cols[mat][color]
        lead = (slice(None),) * (4 - phase)
        slot = (phase - 1) * 6 + mat * 3 + color
        return pltpu.make_async_remote_copy(
            src_ref=sends[phase - 1][mat].at[lead + (pl.ds(lo, hi - lo),)],
            dst_ref=recvs[phase - 1][mat].at[(lax.rem(block, 2),) + lead + (pl.ds(lo, hi - lo),)],
            send_sem=send_sem.at[slot], recv_sem=recv_sem.at[slot, lax.rem(block, 2)],
            device_id=(peers[ORDERS[color][phase - 1]],), device_id_type=MESH)

    def colors(mat):
        return [(color, pl.ds(lo, hi - lo)) for color, (lo, hi) in enumerate(cols[mat])]

    n_dev, per_dev = w2_ref.shape[:2]
    spread = LANES // per_dev

    def lane_part():
        return lax.broadcasted_iota(jnp.int32, (ROWS, LANES), 1) // per_dev

    def group_copies(layer, half):
        return [pltpu.make_async_copy(
            w1_hbm.at[layer, :, pl.ds(pl.multiple_of((dev * n_chunks // spread + half) * LANES, LANES), LANES)],
            w1_group.at[dev], group_sem.at[dev]) for dev in range(n_dev)]

    @pl.when(step == 0)
    def _():
        for copy in group_copies(w1_hbm.shape[0] - 1, 0):
            copy.start()
        barrier = pltpu.get_barrier_semaphore()
        for peer in peers:
            pl.semaphore_signal(barrier, inc=1, device_id=(peer,), device_id_type=MESH)
        load_x = pltpu.make_async_copy(x_hbm.at[1], x_buf, load_sem.at[0])
        load_g = pltpu.make_async_copy(g_hbm, g_buf, load_sem.at[1])
        load_x.start()
        load_g.start()
        acc[...] = jnp.zeros_like(acc)
        load_x.wait()
        load_g.wait()
        pl.semaphore_wait(barrier, 4)

    @pl.when(step == n_chunks)
    def _():
        load_x = pltpu.make_async_copy(x_hbm.at[0], x_buf, load_sem.at[0])
        load_x.start()
        load_x.wait()

    def order_columns(rows, phase, target):
        part = lane_part()
        for tile in range(n_dev // spread):
            merged = None
            for place in range(spread):
                moved = w1_group[tile * spread + place, rows, :].astype(jnp.float32)
                moved = pltpu.roll(moved, lax.rem(place - phase + spread, spread) * per_dev, 1)
                merged = moved if merged is None else jnp.where(part == place, moved, merged)
            target[rows, tile * LANES:(tile + 1) * LANES] = merged.astype(jnp.bfloat16)

    @pl.when(step == 0)
    def _():
        for copy in group_copies(0, 0):
            copy.wait()

        def row_body(block, carry):
            order_columns(pl.ds(pl.multiple_of(block * ROWS, ROWS), ROWS), 0, w1_next)
            return carry
        lax.fori_loop(0, x_buf.shape[1] // ROWS, row_body, 0)

    def advance(mat):
        @pl.when(step >= 4)
        def _():
            block = step - 4
            for color, span in colors(mat):
                copy = axis_copy(3, mat, color, block)
                copy.wait_send()
                copy.wait_recv()
                total = keep3[mat][:, span] + recv3[mat][lax.rem(block, 2), :, span]
                if mat == 1:
                    out2_ref[:, span] = total
                else:
                    keep3[0][:, span] = total
            if mat == 1:
                return
            chunk = lax.rem(block, n_chunks)

            @pl.when(chunk == 0)
            def _():
                out1_ref[...] = jnp.zeros_like(out1_ref)
            phase = lax.rem(chunk, spread)
            part = lax.broadcasted_iota(jnp.int32, (out1_ref.shape[0], LANES), 1) // per_dev
            for dev in range(n_dev):
                tile = dev // spread
                moved = pltpu.roll(keep3[0][:, tile * LANES:(tile + 1) * LANES], lax.rem(phase - dev % spread + spread, spread) * per_dev, 1)
                spot = pl.ds(pl.multiple_of((dev * n_chunks // spread + chunk // spread) * LANES, LANES), LANES)
                out1_ref[:, spot] = jnp.where(part == phase, moved, out1_ref[:, spot])

        @pl.when((step >= 3) & (step < n_steps + 3))
        def _():
            block = step - 3
            for color, span in colors(mat):
                copy = axis_copy(2, mat, color, block)
                copy.wait_send()
                copy.wait_recv()
                bit = bits[ORDERS[color][2]]
                slot = lax.rem(block, 2)
                send3[mat][:, span] = keep2[mat][1 - bit, :, span] + recv2[mat][slot, 1 - bit, :, span]
                keep3[mat][:, span] = keep2[mat][bit, :, span] + recv2[mat][slot, bit, :, span]
                axis_copy(3, mat, color, block).start()

        @pl.when((step >= 2) & (step < n_steps + 2))
        def _():
            block = step - 2
            for color, span in colors(mat):
                copy = axis_copy(1, mat, color, block)
                copy.wait_send()
                copy.wait_recv()
                left = [axis for axis in range(3) if axis != ORDERS[color][0]]
                place = left.index(ORDERS[color][1])
                bit = bits[ORDERS[color][1]]
                slot = lax.rem(block, 2)
                for value, store in ((1 - bit, send2), (bit, keep2)):
                    index = at_bits({place: value}, 2)
                    store[mat][:, :, span] = keep1[mat][index + (slice(None), span)] + recv1[mat][(slot,) + index + (slice(None), span)]
                axis_copy(2, mat, color, block).start()

        @pl.when((step >= 1) & (step < n_steps + 1))
        def _():
            block = step - 1
            copy = core_copy(mat, block)
            copy.wait_send()
            copy.wait_recv()
            for color, span in colors(mat):
                axis = ORDERS[color][0]
                slot = lax.rem(block, 2)
                for value, store in ((1 - bits[axis], send1), (bits[axis], keep1)):
                    index = at_bits({axis: value}, 3)
                    mine = parts[mat][index + (bits[3], slice(None), span)].astype(jnp.float32)
                    store[mat][:, :, :, span] = mine + recv0[mat][(slot,) + index + (slice(None), span)].astype(jnp.float32)
                axis_copy(1, mat, color, block).start()

    advance(0)

    @pl.when(step < n_steps)
    def _():
        w1_ref[...] = w1_next[...]

    @pl.when((step < n_steps - 1) & (lax.rem(step, spread) == spread - 1))
    def _():
        for copy in group_copies(0, 0):
            copy.wait()

    def tile_body(tile, turn_x):
        rows = pl.ds(pl.multiple_of(tile * TILE_B, TILE_B), TILE_B)
        pre = jnp.dot(x_buf[rows, :], w1_ref[...], preferred_element_type=jnp.float32)
        d_act = dot_nt(g_buf[rows, :], w2_ref[...].reshape(w1_ref.shape[1], w1_ref.shape[0]))
        square = pre * pre
        gate = 0.5 + 0.5 * jnp.tanh(pre * (GELU_A + GELU_B * square))
        act = pre * gate
        act_turned[:, rows] = act.astype(jnp.bfloat16).T
        slope = gate + (act * (1.0 - gate)) * (2.0 * GELU_A + 6.0 * GELU_B * square)
        dh_buf[rows, :] = (d_act * slope).astype(jnp.bfloat16)
        if turn_x:
            x_turned[:, rows] = x_buf[rows, :].T

    first = lax.rem(step, n_chunks) == 0

    @pl.when((step < n_steps) & first)
    def _():
        lax.fori_loop(0, tokens // TILE_B, lambda tile, carry: (tile_body(tile, True), carry)[1], 0)

    @pl.when((step < n_steps) & (lax.rem(step, n_chunks) > 0))
    def _():
        lax.fori_loop(0, tokens // TILE_B, lambda tile, carry: (tile_body(tile, False), carry)[1], 0)

    @pl.when(step < n_steps)
    def _():
        for block in range(w1_next.shape[0] // ROWS):
            order_columns(pl.ds(block * ROWS, ROWS), lax.rem(step + 1, spread), w1_next)
        part1[...] = jnp.dot(x_turned[...], dh_buf[...], preferred_element_type=jnp.float32).astype(jnp.bfloat16).reshape(part1.shape)
        core_copy(0, step).start()

    @pl.when((step < n_steps - 2) & (lax.rem(step, spread) == spread - 2))
    def _():
        following = step + 2
        for copy in group_copies(w1_hbm.shape[0] - 1 - following // n_chunks, lax.rem(following, n_chunks) // spread):
            copy.start()

    advance(1)

    @pl.when(step < n_steps)
    def _():
        part2[...] = jnp.dot(act_turned[...], g_buf[...], preferred_element_type=jnp.float32).astype(jnp.bfloat16).reshape(part2.shape)
        core_copy(1, step).start()

    @pl.when(step < n_chunks)
    def _():
        def tile_body(tile, carry):
            rows = pl.ds(pl.multiple_of(tile * TILE, TILE), TILE)
            acc[rows, :] += dot_nt(dh_buf[rows, :], w1_ref[...])
            return carry
        lax.fori_loop(0, tokens // TILE, tile_body, 0)

    @pl.when(step == n_chunks - 1)
    def _():
        def tile_body(tile, carry):
            rows = pl.ds(pl.multiple_of(tile * TILE, TILE), TILE)
            g_buf[rows, :] = (g_buf[rows, :].astype(jnp.float32) + acc[rows, :]).astype(jnp.bfloat16)
            return carry
        lax.fori_loop(0, tokens // TILE, tile_body, 0)


def backward_sums(x_tokens, grad_tokens, w_up, w_down, n_dev):
    layers, model_width, ff_width = w_up.shape
    tokens = grad_tokens.shape[0]
    chunk = 512
    n_chunks = ff_width // chunk
    per_dev = chunk // n_dev
    rows_up = model_width // n_dev
    n_steps = layers * n_chunks
    cols = (((0, chunk // 4), (chunk // 4, chunk // 2), (chunk // 2, chunk)), ((0, 384), (384, 768), (768, model_width)))
    w2_view = w_down.reshape(layers, n_dev, n_chunks, per_dev, model_width)

    def where(step):
        last = jnp.minimum(step, n_steps - 1)
        return layers - 1 - last // n_chunks, lax.rem(last, n_chunks)

    def pair(lead, dtype):
        return [pltpu.VMEM(lead + (rows_up, chunk), dtype), pltpu.VMEM(lead + (per_dev, model_width), dtype)]

    f32, b16 = jnp.float32, jnp.bfloat16
    scratch = [pltpu.VMEM((tokens, model_width), b16), pltpu.VMEM((tokens, model_width), b16), pltpu.VMEM((model_width, tokens), b16),
               pltpu.VMEM((tokens, model_width), f32), pltpu.VMEM((chunk, tokens), b16), pltpu.VMEM((tokens, chunk), b16),
               pltpu.VMEM((n_dev, model_width, LANES), b16), pltpu.VMEM((model_width, chunk), b16), pltpu.VMEM((model_width, chunk), b16)]
    scratch += pair((2, 2, 2, 2), b16) + pair((2, 2, 2, 2), b16)
    for lead in ((2, 2), (2,), ()):
        scratch += pair(lead, f32) + pair(lead, f32) + pair((2,) + lead, f32)
    dma = pltpu.SemaphoreType.DMA
    scratch += [dma((2,)), dma((n_dev,)), dma((2,)), dma((2, 2)), dma((18,)), dma((18, 2))]
    hbm = pl.BlockSpec(memory_space=pl.ANY)
    out1, out2 = pl.pallas_call(
        functools.partial(backward_kernel, n_steps, n_chunks, cols),
        grid=(n_steps + 4,),
        in_specs=[hbm, hbm,
                  hbm,
                  pl.BlockSpec((None, n_dev, None, per_dev, model_width), lambda s: (where(s)[0], 0, where(s)[1], 0, 0))],
        out_specs=[pl.BlockSpec((None, rows_up, ff_width), lambda s: (where(jnp.maximum(s - 4, 0))[0], 0, 0)),
                   pl.BlockSpec((None, per_dev, model_width), lambda s: (*where(jnp.maximum(s - 4, 0)), 0))],
        out_shape=[jax.ShapeDtypeStruct((layers, rows_up, ff_width), f32), jax.ShapeDtypeStruct((layers, n_chunks * per_dev, model_width), f32)],
        scratch_shapes=scratch,
        compiler_params=pltpu.CompilerParams(vmem_limit_bytes=67_043_328, dimension_semantics=("arbitrary",), collective_id=0, has_side_effects=True),
        cost_estimate=pl.CostEstimate(flops=18 * tokens * model_width * ff_width, bytes_accessed=60_000_000, transcendentals=2 * tokens * ff_width),
        name="backward_reduce",
    )(x_tokens, grad_tokens, w_up, w2_view)
    return out1, out2


def norm_kernel(n_dev, value_ref, out_ref, gathered, send_sem, recv_sem):
    me = lax.axis_index("fsdp")
    barrier = pltpu.get_barrier_semaphore()
    for shift in range(1, n_dev):
        pl.semaphore_signal(barrier, inc=1, device_id=(lax.rem(me + shift, n_dev),), device_id_type=MESH)
    pl.semaphore_wait(barrier, n_dev - 1)

    def copy_of(shift, sender):
        return pltpu.make_async_remote_copy(
            src_ref=value_ref, dst_ref=gathered.at[sender], send_sem=send_sem.at[shift], recv_sem=recv_sem.at[sender],
            device_id=(lax.rem(me + shift, n_dev),), device_id_type=MESH)

    for shift in range(1, n_dev):
        copy_of(shift, me).start()
    gathered[me] = value_ref[...]
    for shift in range(1, n_dev):
        copy_of(shift, lax.rem(me + n_dev - shift, n_dev)).wait_recv()
    total = gathered[0]
    for dev in range(1, n_dev):
        total = total + gathered[dev]
    out_ref[...] = total
    for shift in range(1, n_dev):
        copy_of(shift, me).wait_send()


def global_sum(value, n_dev):
    tile = jnp.broadcast_to(value, (8, LANES))
    vmem = pl.BlockSpec(memory_space=pltpu.VMEM)
    dma = pltpu.SemaphoreType.DMA
    return pl.pallas_call(
        functools.partial(norm_kernel, n_dev), in_specs=[vmem], out_specs=vmem,
        out_shape=jax.ShapeDtypeStruct(tile.shape, jnp.float32),
        scratch_shapes=[pltpu.VMEM((n_dev,) + tile.shape, jnp.float32), dma((n_dev,)), dma((n_dev,))],
        compiler_params=pltpu.CompilerParams(collective_id=1, has_side_effects=True),
        name="norm_sum")(tile)[0, 0]


def forward_kernel(x_hbm, up0_hbm, down0_hbm, up1_hbm, down1_hbm, y_hbm, h_buf, act_buf, buf_a, buf_b, buf_c, load_sem, free_sem, send_sem, recv_sem):
    shards = (up0_hbm, down0_hbm, up1_hbm, down1_hbm)
    bufs = (buf_a, buf_b, buf_c, buf_a)
    me = lax.axis_index("fsdp")
    bits = [lax.rem(me // stride, 2) for stride in STRIDES]
    peers = [me + (1 - 2 * bit) * stride for bit, stride in zip(bits, STRIDES)]
    rows = up0_hbm.shape[0]
    tokens, width = h_buf.shape
    quarter = rows // 4
    pieces = ((0, 0, rows // 2), (0, rows // 2, rows), (1, 0, rows), (2, 0, rows), (3, 0, rows))
    n_tiles = tokens // TILE

    def spans(piece):
        _, lo, hi = pieces[piece]
        size = (hi - lo) // 16
        third = size // 3
        cuts = [0, third, 2 * third, size]
        if piece % 3 == 1:
            cuts = [0, third, size - third, size]
        if piece % 3 == 2:
            cuts = [0, size - 2 * third, size - third, size]
        return [(lo + 16 * cuts[color], 16 * (cuts[color + 1] - cuts[color])) for color in range(3)]

    def copies(piece, phase):
        matrix = pieces[piece][0]
        out = []
        for color, (lo, size) in enumerate(spans(piece)):
            order = ORDERS[color]
            picks = {axis: bits[axis] for axis in range(4)}
            for axis in order[:min(phase, 2)]:
                picks.pop(axis)
            if phase == 4:
                picks[order[2]] = 1 - bits[order[2]]
            where = at_bits(picks, 4) + (pl.ds(lo, size),)
            axis = order[phase] if phase < 3 else 3
            slot = (piece * 5 + phase) * 3 + color
            out.append(pltpu.make_async_remote_copy(
                src_ref=bufs[matrix].at[where], dst_ref=bufs[matrix].at[where],
                send_sem=send_sem.at[slot], recv_sem=recv_sem.at[slot],
                device_id=(peers[axis],), device_id_type=MESH))
        return out

    def start(piece, phase):
        for copy in copies(piece, phase):
            copy.start()

    def arrived(piece, phase):
        for copy in copies(piece, phase):
            copy.wait_recv()

    def second(piece):
        arrived(piece, 0)
        start(piece, 1)

    def third(piece):
        arrived(piece, 1)
        start(piece, 2)
        start(piece, 3)

    def hand_over(piece):
        arrived(piece, 2)
        start(piece, 4)

    def complete(piece):
        arrived(piece, 3)
        arrived(piece, 4)

    def load(matrix):
        return pltpu.make_async_copy(shards[matrix], bufs[matrix].at[tuple(bits)], load_sem.at[matrix])

    barrier = pltpu.get_barrier_semaphore()
    for peer in peers:
        pl.semaphore_signal(barrier, inc=1, device_id=(peer,), device_id_type=MESH)
    for matrix in range(3):
        load(matrix).start()
    load_x = pltpu.make_async_copy(x_hbm, h_buf, load_sem.at[4])
    load_x.start()
    load(0).wait()
    pl.semaphore_wait(barrier, 4)
    start(0, 0)
    start(1, 0)
    load(1).wait()
    load(2).wait()
    second(0)
    start(2, 0)
    second(1)
    third(0)
    second(2)
    start(3, 0)
    third(1)
    hand_over(0)
    load_x.wait()
    complete(0)

    def weights(matrix, block):
        return bufs[matrix][:, :, :, :, pl.ds(pl.multiple_of(block * quarter, quarter), quarter), :].reshape(4 * 4 * quarter, width)

    def run(count, matrix, body, events):
        def step(index, carry):
            for when, event in events.items():
                pl.when(index == when)(event)
            body(index, matrix)
            return carry
        lax.fori_loop(0, count, step, 0)

    def up(index, matrix):
        block, tile = index // n_tiles, lax.rem(index, n_tiles)
        span = pl.ds(pl.multiple_of(tile * TILE, TILE), TILE)
        pre = jnp.dot(h_buf[span, :], weights(matrix, block), preferred_element_type=jnp.float32)
        gate = 0.5 + 0.5 * jnp.tanh(pre * (GELU_A + GELU_B * (pre * pre)))
        act_buf[block, span, :] = (pre * gate).astype(jnp.bfloat16)

    def down(tile, matrix):
        span = pl.ds(pl.multiple_of(tile * TILE, TILE), TILE)
        total = h_buf[span, :].astype(jnp.float32)
        for block in range(4):
            total = total + jnp.dot(act_buf[block, span, :], bufs[matrix][block // 2, block % 2].reshape(width, width), preferred_element_type=jnp.float32)
        h_buf[span, :] = total.astype(jnp.bfloat16)

    def store(tile):
        span = pl.ds(pl.multiple_of(tile * TILE, TILE), TILE)
        return pltpu.make_async_copy(h_buf.at[span, :], y_hbm.at[span, :], load_sem.at[5 + tile])

    def down_last(tile, matrix):
        down(tile, matrix)
        store(tile).start()

    def widen_both():
        second(3)
        third(2)

    run(4 * n_tiles, 0, up, {3: widen_both, 2 * n_tiles - 3: lambda: hand_over(1), 2 * n_tiles: lambda: complete(1),
                             3 * n_tiles: lambda: third(3), 4 * n_tiles - 1: lambda: hand_over(2)})
    for piece in (0, 1):
        for phase in range(5):
            for copy in copies(piece, phase):
                copy.wait_send()
    for peer in peers:
        pl.semaphore_signal(free_sem, inc=1, device_id=(peer,), device_id_type=MESH)
    load(3).start()
    complete(2)
    load(3).wait()
    pl.semaphore_wait(free_sem, 4)
    start(4, 0)
    run(n_tiles, 1, down, {n_tiles - 2: lambda: hand_over(3), n_tiles - 1: lambda: second(4)})
    complete(3)
    run(4 * n_tiles, 2, up, {n_tiles: lambda: third(4), 4 * n_tiles - 2: lambda: hand_over(4)})
    complete(4)
    run(n_tiles, 3, down_last, {})
    for piece in (2, 3, 4):
        for phase in range(5):
            for copy in copies(piece, phase):
                copy.wait_send()
    for tile in range(n_tiles):
        store(tile).wait()


def forward_stack(x_tokens, up_shard, down_shard, n_dev):
    tokens, model_width = x_tokens.shape
    layers, rows, ff_width = up_shard.shape
    blocks = ff_width // model_width
    up_blocks = up_shard.reshape(layers, rows, blocks, model_width).transpose(0, 2, 1, 3).reshape(layers, blocks * rows, model_width)
    hbm = pl.BlockSpec(memory_space=pl.ANY)
    b16 = jnp.bfloat16
    gathered = pltpu.VMEM((2, 2, 2, 2, blocks * rows, model_width), b16)
    dma = pltpu.SemaphoreType.DMA
    return pl.pallas_call(
        forward_kernel, in_specs=[hbm] * 5, out_specs=hbm,
        out_shape=jax.ShapeDtypeStruct((tokens, model_width), b16),
        scratch_shapes=[pltpu.VMEM((tokens, model_width), b16), pltpu.VMEM((blocks, tokens, model_width), b16), gathered, gathered, gathered,
                        dma((5 + tokens // TILE,)), pltpu.SemaphoreType.REGULAR, dma((75,)), dma((75,))],
        compiler_params=pltpu.CompilerParams(vmem_limit_bytes=67_043_328, collective_id=2, has_side_effects=True),
        cost_estimate=pl.CostEstimate(flops=8 * tokens * model_width * ff_width, bytes_accessed=20_000_000, transcendentals=2 * tokens * ff_width),
        name="gather_forward",
    )(x_tokens, up_blocks[0], down_shard[0], up_blocks[1], down_shard[1])


def solution(mesh):
    n_dev = mesh.shape["fsdp"]
    rows_spec = P(None, "fsdp")

    def local_step(x_saved, grad_out, x_next, w_up, w_down, gacc_up, gacc_down, master_up, master_down, mom1_up, mom1_down, mom2_up, mom2_down):
        layers, model_width, ff_width = w_up.shape
        clip_norm = 0.1 * math.sqrt(2 * layers * model_width * ff_width)
        sums_up, sums_down = backward_sums(x_saved.reshape(layers, -1, model_width), grad_out.reshape(-1, model_width), w_up, w_down, n_dev)
        grad_up = (gacc_up + sums_up) / MICRO_STEPS
        grad_down = (gacc_down + sums_down) / MICRO_STEPS
        local_sq = jnp.sum(grad_up * grad_up) + jnp.sum(grad_down * grad_down)
        clip_factor = jnp.minimum(1.0, clip_norm / jnp.sqrt(global_sum(local_sq, n_dev)))
        new_up = adamw_update(master_up, mom1_up, mom2_up, grad_up * clip_factor)
        new_down = adamw_update(master_down, mom1_down, mom2_down, grad_down * clip_factor)
        up_shard = new_up[0].astype(jnp.bfloat16)
        down_shard = new_down[0].astype(jnp.bfloat16)
        hidden_state = forward_stack(x_next.reshape(-1, model_width), up_shard, down_shard, n_dev)
        return (hidden_state.reshape(x_next.shape), new_up[0], new_down[0], new_up[1], new_down[1], new_up[2], new_down[2])

    return jax.shard_map(local_step, mesh=mesh, in_specs=(rows_spec, P("fsdp"), P("fsdp"), P(), P(), rows_spec, rows_spec, rows_spec, rows_spec, rows_spec, rows_spec, rows_spec, rows_spec), out_specs=(P("fsdp"), rows_spec, rows_spec, rows_spec, rows_spec, rows_spec, rows_spec), check_vma=False)
```

```python
import functools
import math
import jax
import jax.numpy as jnp
from jax import lax
from jax.experimental import pallas as pl
from jax.experimental.pallas import tpu as pltpu
from jax.sharding import PartitionSpec as P

LEARN_RATE = 0.001
BETA_ONE = 0.9
BETA_TWO = 0.95
ADAM_EPS = 1e-8
WEIGHT_DECAY = 0.1
ADAM_STEP = 3

GELU_A = math.sqrt(2.0 / math.pi)
GELU_B = GELU_A * 0.044715
MESH = pl.DeviceIdType.MESH
STRIDES = (8, 4, 2, 1)
ORDERS = ((2, 1, 0), (1, 0, 2), (0, 2, 1))
TILE = 512
LANES = 128
ROWS = 128
TILE_B = 512


def adamw_update(master_old, mom_one, mom_two, grad_clip):
    mom_one_new = BETA_ONE * mom_one + (1.0 - BETA_ONE) * grad_clip
    mom_two_new = BETA_TWO * mom_two + (1.0 - BETA_TWO) * grad_clip * grad_clip
    first_hat = mom_one_new / (1.0 - BETA_ONE ** ADAM_STEP)
    second_hat = mom_two_new / (1.0 - BETA_TWO ** ADAM_STEP)
    master_new = master_old - LEARN_RATE * (first_hat / (jnp.sqrt(second_hat) + ADAM_EPS) + WEIGHT_DECAY * master_old)
    return master_new, mom_one_new, mom_two_new


def dot_nt(left, right):
    return lax.dot_general(left, right, (((1,), (1,)), ((), ())), preferred_element_type=jnp.float32)


def at_bits(picks, count):
    return tuple(picks.get(dim, slice(None)) for dim in range(count))


def backward_kernel(n_steps, n_chunks, cols, x_hbm, g_hbm, w1_hbm, w2_ref, gacc1_hbm, gacc2_ref, out1_block, out2_ref, norm_ref, x_buf, g_buf, x_turned, acc, act_turned, dh_buf, w1_group, w1_ref, w1_next, part1, part2, *rest):
    parts = (part1, part2)
    out1_ref = out1_block.at[0]
    recv0, send1, keep1, recv1, send2, keep2, recv2, send3, keep3, recv3 = (rest[2 * i:2 * i + 2] for i in range(10))
    squares, gathered, load_sem, group_sem, send_sem0, recv_sem0, send_sem, recv_sem, norm_send, norm_recv = rest[20:]
    step = pl.program_id(0)
    me = lax.axis_index("fsdp")
    bits = [lax.rem(me // stride, 2) for stride in STRIDES]
    peers = [me + (1 - 2 * bit) * stride for bit, stride in zip(bits, STRIDES)]
    tokens = x_buf.shape[0]
    sends = (send1, send2, send3)
    recvs = (recv1, recv2, recv3)

    def core_copy(mat, block):
        return pltpu.make_async_remote_copy(
            src_ref=parts[mat].at[:, :, :, 1 - bits[3]], dst_ref=recv0[mat].at[lax.rem(block, 2)],
            send_sem=send_sem0.at[mat], recv_sem=recv_sem0.at[mat, lax.rem(block, 2)],
            device_id=(peers[3],), device_id_type=MESH)

    def axis_copy(phase, mat, color, block):
        lo, hi = cols[mat][color]
        lead = (slice(None),) * (4 - phase)
        slot = (phase - 1) * 6 + mat * 3 + color
        return pltpu.make_async_remote_copy(
            src_ref=sends[phase - 1][mat].at[lead + (pl.ds(lo, hi - lo),)],
            dst_ref=recvs[phase - 1][mat].at[(lax.rem(block, 2),) + lead + (pl.ds(lo, hi - lo),)],
            send_sem=send_sem.at[slot], recv_sem=recv_sem.at[slot, lax.rem(block, 2)],
            device_id=(peers[ORDERS[color][phase - 1]],), device_id_type=MESH)

    def colors(mat):
        return [(color, pl.ds(lo, hi - lo)) for color, (lo, hi) in enumerate(cols[mat])]

    n_dev, per_dev = w2_ref.shape[:2]
    spread = LANES // per_dev

    def lane_part():
        return lax.broadcasted_iota(jnp.int32, (ROWS, LANES), 1) // per_dev

    def group_copies(layer, half):
        return [pltpu.make_async_copy(
            w1_hbm.at[layer, :, pl.ds(pl.multiple_of((dev * n_chunks // spread + half) * LANES, LANES), LANES)],
            w1_group.at[dev], group_sem.at[dev]) for dev in range(n_dev)]

    def order_columns(rows, phase, target):
        part = lane_part()
        for tile in range(n_dev // spread):
            merged = None
            for place in range(spread):
                moved = w1_group[tile * spread + place, rows, :].astype(jnp.float32)
                moved = pltpu.roll(moved, lax.rem(place - phase + spread, spread) * per_dev, 1)
                merged = moved if merged is None else jnp.where(part == place, moved, merged)
            target[rows, tile * LANES:(tile + 1) * LANES] = merged.astype(jnp.bfloat16)

    @pl.when(step == 0)
    def _():
        for copy in group_copies(w1_hbm.shape[0] - 1, 0):
            copy.start()
        load_x = pltpu.make_async_copy(x_hbm.at[w1_hbm.shape[0] - 1], x_buf, load_sem.at[0])
        load_g = pltpu.make_async_copy(g_hbm, g_buf, load_sem.at[1])
        load_x.start()
        load_g.start()
        barrier = pltpu.get_barrier_semaphore()
        for shift in range(1, n_dev):
            pl.semaphore_signal(barrier, inc=1, device_id=(lax.rem(me + shift, n_dev),), device_id_type=MESH)
        acc[...] = jnp.zeros_like(acc)
        squares[...] = jnp.zeros_like(squares)
        for copy in group_copies(0, 0):
            copy.wait()

        def row_body(block, carry):
            order_columns(pl.ds(pl.multiple_of(block * ROWS, ROWS), ROWS), 0, w1_next)
            return carry
        lax.fori_loop(0, x_buf.shape[1] // ROWS, row_body, 0)
        load_x.wait()
        load_g.wait()
        pl.semaphore_wait(barrier, n_dev - 1)

    def next_x():
        return pltpu.make_async_copy(x_hbm.at[0], x_buf, load_sem.at[0])

    @pl.when(step == n_chunks)
    def _():
        next_x().wait()

    def add_squares(grad):
        total = squares[...]
        for row in range(0, grad.shape[0], 8):
            for lane in range(0, grad.shape[1], LANES):
                piece = grad[row:row + 8, lane:lane + LANES]
                total = total + piece * piece
        squares[...] = total

    def advance(mat):
        @pl.when(step >= 4)
        def _():
            block = step - 4
            for color, span in colors(mat):
                copy = axis_copy(3, mat, color, block)
                copy.wait_send()
                copy.wait_recv()
                total = keep3[mat][:, span] + recv3[mat][lax.rem(block, 2), :, span]
                if mat == 1:
                    grad = 0.5 * (gacc2_ref[:, span] + total)
                    out2_ref[:, span] = grad
                    add_squares(grad)
                else:
                    keep3[0][:, span] = total
            if mat == 1:
                return
            chunk = lax.rem(block, n_chunks)

            @pl.when(chunk == 0)
            def _():
                load = pltpu.make_async_copy(gacc1_hbm.at[w1_hbm.shape[0] - 1 - block // n_chunks], out1_ref, load_sem.at[2])
                load.start()
                load.wait()
            phase = lax.rem(chunk, spread)
            part = lax.broadcasted_iota(jnp.int32, (out1_ref.shape[0], LANES), 1) // per_dev
            for dev in range(n_dev):
                tile = dev // spread
                moved = pltpu.roll(keep3[0][:, tile * LANES:(tile + 1) * LANES], lax.rem(phase - dev % spread + spread, spread) * per_dev, 1)
                spot = pl.ds(pl.multiple_of((dev * n_chunks // spread + chunk // spread) * LANES, LANES), LANES)
                out1_ref[:, spot] = jnp.where(part == phase, 0.5 * (out1_ref[:, spot] + moved), out1_ref[:, spot])

            @pl.when(chunk == n_chunks - 1)
            def _():
                add_squares(out1_ref[...])

        @pl.when((step >= 3) & (step < n_steps + 3))
        def _():
            block = step - 3
            for color, span in colors(mat):
                copy = axis_copy(2, mat, color, block)
                copy.wait_send()
                copy.wait_recv()
                bit = bits[ORDERS[color][2]]
                slot = lax.rem(block, 2)
                send3[mat][:, span] = keep2[mat][1 - bit, :, span] + recv2[mat][slot, 1 - bit, :, span]
                keep3[mat][:, span] = keep2[mat][bit, :, span] + recv2[mat][slot, bit, :, span]
                axis_copy(3, mat, color, block).start()

        @pl.when((step >= 2) & (step < n_steps + 2))
        def _():
            block = step - 2
            for color, span in colors(mat):
                copy = axis_copy(1, mat, color, block)
                copy.wait_send()
                copy.wait_recv()
                left = [axis for axis in range(3) if axis != ORDERS[color][0]]
                place = left.index(ORDERS[color][1])
                bit = bits[ORDERS[color][1]]
                slot = lax.rem(block, 2)
                for value, store in ((1 - bit, send2), (bit, keep2)):
                    index = at_bits({place: value}, 2)
                    store[mat][:, :, span] = keep1[mat][index + (slice(None), span)] + recv1[mat][(slot,) + index + (slice(None), span)]
                axis_copy(2, mat, color, block).start()

        @pl.when((step >= 1) & (step < n_steps + 1))
        def _():
            block = step - 1
            copy = core_copy(mat, block)
            copy.wait_send()
            copy.wait_recv()
            for color, span in colors(mat):
                axis = ORDERS[color][0]
                slot = lax.rem(block, 2)
                for value, store in ((1 - bits[axis], send1), (bits[axis], keep1)):
                    index = at_bits({axis: value}, 3)
                    mine = parts[mat][index + (bits[3], slice(None), span)].astype(jnp.float32)
                    store[mat][:, :, :, span] = mine + recv0[mat][(slot,) + index + (slice(None), span)].astype(jnp.float32)
                axis_copy(1, mat, color, block).start()

    advance(0)

    @pl.when(step < n_steps)
    def _():
        w1_ref[...] = w1_next[...]

    @pl.when((step < n_steps - 1) & (lax.rem(step, spread) == spread - 1))
    def _():
        for copy in group_copies(0, 0):
            copy.wait()

    def tile_body(tile, turn_x):
        rows = pl.ds(pl.multiple_of(tile * TILE_B, TILE_B), TILE_B)
        pre = jnp.dot(x_buf[rows, :], w1_ref[...], preferred_element_type=jnp.float32)
        d_act = dot_nt(g_buf[rows, :], w2_ref[...].reshape(w1_ref.shape[1], w1_ref.shape[0]))
        square = pre * pre
        gate = 0.5 + 0.5 * jnp.tanh(pre * (GELU_A + GELU_B * square))
        act = pre * gate
        act_turned[:, rows] = act.astype(jnp.bfloat16).T
        slope = gate + (act * (1.0 - gate)) * (2.0 * GELU_A + 6.0 * GELU_B * square)
        dh_buf[rows, :] = (d_act * slope).astype(jnp.bfloat16)
        if turn_x:
            x_turned[:, rows] = x_buf[rows, :].T

    first = lax.rem(step, n_chunks) == 0

    @pl.when((step < n_steps) & first)
    def _():
        lax.fori_loop(0, tokens // TILE_B, lambda tile, carry: (tile_body(tile, True), carry)[1], 0)

    @pl.when((step < n_steps) & (lax.rem(step, n_chunks) > 0))
    def _():
        lax.fori_loop(0, tokens // TILE_B, lambda tile, carry: (tile_body(tile, False), carry)[1], 0)

    @pl.when(step < n_steps)
    def _():
        for block in range(w1_next.shape[0] // ROWS):
            order_columns(pl.ds(block * ROWS, ROWS), lax.rem(step + 1, spread), w1_next)
        part1[...] = jnp.dot(x_turned[...], dh_buf[...], preferred_element_type=jnp.float32).astype(jnp.bfloat16).reshape(part1.shape)
        core_copy(0, step).start()

    @pl.when(step == n_chunks - 1)
    def _():
        next_x().start()

    @pl.when((step < n_steps - 2) & (lax.rem(step, spread) == spread - 2))
    def _():
        following = step + 2
        for copy in group_copies(w1_hbm.shape[0] - 1 - following // n_chunks, lax.rem(following, n_chunks) // spread):
            copy.start()

    advance(1)

    @pl.when(step < n_steps)
    def _():
        part2[...] = jnp.dot(act_turned[...], g_buf[...], preferred_element_type=jnp.float32).astype(jnp.bfloat16).reshape(part2.shape)
        core_copy(1, step).start()

    @pl.when(step < n_chunks)
    def _():
        def tile_body(tile, carry):
            rows = pl.ds(pl.multiple_of(tile * TILE, TILE), TILE)
            acc[rows, :] += dot_nt(dh_buf[rows, :], w1_ref[...])
            return carry
        lax.fori_loop(0, tokens // TILE, tile_body, 0)

    @pl.when(step == n_chunks - 1)
    def _():
        def tile_body(tile, carry):
            rows = pl.ds(pl.multiple_of(tile * TILE, TILE), TILE)
            g_buf[rows, :] = (g_buf[rows, :].astype(jnp.float32) + acc[rows, :]).astype(jnp.bfloat16)
            return carry
        lax.fori_loop(0, tokens // TILE, tile_body, 0)

    @pl.when(step == n_steps + 3)
    def _():
        def copy_of(shift, sender):
            return pltpu.make_async_remote_copy(
                src_ref=squares, dst_ref=gathered.at[sender], send_sem=norm_send.at[shift], recv_sem=norm_recv.at[sender],
                device_id=(lax.rem(me + shift, n_dev),), device_id_type=MESH)

        for shift in range(1, n_dev):
            copy_of(shift, me).start()
        gathered[me] = squares[...]
        for shift in range(1, n_dev):
            copy_of(shift, lax.rem(me + n_dev - shift, n_dev)).wait_recv()
        total = gathered[0]
        for dev in range(1, n_dev):
            total = total + gathered[dev]
        norm_ref[...] = jnp.broadcast_to(jnp.sum(total, keepdims=True), norm_ref.shape)
        for shift in range(1, n_dev):
            copy_of(shift, me).wait_send()


def backward_grads(x_tokens, grad_tokens, w_up, w_down, gacc_up, gacc_down, n_dev):
    layers, model_width, ff_width = w_up.shape
    tokens = grad_tokens.shape[0]
    chunk = 512
    n_chunks = ff_width // chunk
    per_dev = chunk // n_dev
    rows_up = model_width // n_dev
    n_steps = layers * n_chunks
    cols = (((0, chunk // 4), (chunk // 4, chunk // 2), (chunk // 2, chunk)), ((0, 384), (384, 768), (768, model_width)))
    w2_view = w_down.reshape(layers, n_dev, n_chunks, per_dev, model_width)

    def where(step):
        last = jnp.minimum(step, n_steps - 1)
        return layers - 1 - last // n_chunks, lax.rem(last, n_chunks)

    def pair(lead, dtype):
        return [pltpu.VMEM(lead + (rows_up, chunk), dtype), pltpu.VMEM(lead + (per_dev, model_width), dtype)]

    f32, b16 = jnp.float32, jnp.bfloat16
    scratch = [pltpu.VMEM((tokens, model_width), b16), pltpu.VMEM((tokens, model_width), b16), pltpu.VMEM((model_width, tokens), b16),
               pltpu.VMEM((tokens, model_width), f32), pltpu.VMEM((chunk, tokens), b16), pltpu.VMEM((tokens, chunk), b16),
               pltpu.VMEM((n_dev, model_width, LANES), b16), pltpu.VMEM((model_width, chunk), b16), pltpu.VMEM((model_width, chunk), b16)]
    scratch += pair((2, 2, 2, 2), b16) + pair((2, 2, 2, 2), b16)
    for lead in ((2, 2), (2,), ()):
        scratch += pair(lead, f32) + pair(lead, f32) + pair((2,) + lead, f32)
    dma = pltpu.SemaphoreType.DMA
    scratch += [pltpu.VMEM((8, LANES), f32), pltpu.VMEM((n_dev, 8, LANES), f32)]
    scratch += [dma((3,)), dma((n_dev,)), dma((2,)), dma((2, 2)), dma((18,)), dma((18, 2)), dma((n_dev,)), dma((n_dev,))]
    hbm = pl.BlockSpec(memory_space=pl.ANY)
    grad_up, grad_down, norm_sq = pl.pallas_call(
        functools.partial(backward_kernel, n_steps, n_chunks, cols),
        grid=(n_steps + 4,),
        in_specs=[hbm, hbm,
                  hbm,
                  pl.BlockSpec((None, n_dev, None, per_dev, model_width), lambda s: (where(s)[0], 0, where(s)[1], 0, 0)),
                  hbm, pl.BlockSpec((None, per_dev, model_width), lambda s: (*where(jnp.maximum(s - 4, 0)), 0))],
        out_specs=[pl.BlockSpec((1, rows_up, ff_width), lambda s: (where(jnp.maximum(s - 4, 0))[0], 0, 0)),
                   pl.BlockSpec((None, per_dev, model_width), lambda s: (*where(jnp.maximum(s - 4, 0)), 0)),
                   pl.BlockSpec((8, LANES), lambda s: (0, 0))],
        out_shape=[jax.ShapeDtypeStruct((layers, rows_up, ff_width), f32), jax.ShapeDtypeStruct((layers, n_chunks * per_dev, model_width), f32),
                   jax.ShapeDtypeStruct((8, LANES), f32)],
        scratch_shapes=scratch,
        compiler_params=pltpu.CompilerParams(vmem_limit_bytes=67_043_328, dimension_semantics=("arbitrary",), collective_id=0, has_side_effects=True),
        cost_estimate=pl.CostEstimate(flops=18 * tokens * model_width * ff_width, bytes_accessed=60_000_000, transcendentals=2 * tokens * ff_width),
        name="backward_reduce",
    )(x_tokens, grad_tokens, w_up, w2_view, gacc_up, gacc_down)
    return grad_up, grad_down, norm_sq[0, 0]


def forward_kernel(x_hbm, up0_hbm, down0_hbm, up1_hbm, down1_hbm, y_hbm, h_buf, act_buf, buf_a, buf_b, buf_c, load_sem, free_sem, send_sem, recv_sem):
    shards = (up0_hbm, down0_hbm, up1_hbm, down1_hbm)
    bufs = (buf_a, buf_b, buf_c, buf_a)
    me = lax.axis_index("fsdp")
    bits = [lax.rem(me // stride, 2) for stride in STRIDES]
    peers = [me + (1 - 2 * bit) * stride for bit, stride in zip(bits, STRIDES)]
    rows = up0_hbm.shape[0]
    tokens, width = h_buf.shape
    quarter = rows // 4
    pieces = ((0, 0, rows // 2), (0, rows // 2, rows), (1, 0, rows), (2, 0, rows), (3, 0, rows))
    n_tiles = tokens // TILE

    def spans(piece):
        _, lo, hi = pieces[piece]
        size = (hi - lo) // 16
        third = size // 3
        cuts = [0, third, 2 * third, size]
        if piece % 3 == 1:
            cuts = [0, third, size - third, size]
        if piece % 3 == 2:
            cuts = [0, size - 2 * third, size - third, size]
        return [(lo + 16 * cuts[color], 16 * (cuts[color + 1] - cuts[color])) for color in range(3)]

    def copies(piece, phase):
        matrix = pieces[piece][0]
        out = []
        for color, (lo, size) in enumerate(spans(piece)):
            order = ORDERS[color]
            picks = {axis: bits[axis] for axis in range(4)}
            for axis in order[:min(phase, 2)]:
                picks.pop(axis)
            if phase == 4:
                picks[order[2]] = 1 - bits[order[2]]
            where = at_bits(picks, 4) + (pl.ds(lo, size),)
            axis = order[phase] if phase < 3 else 3
            slot = (piece * 5 + phase) * 3 + color
            out.append(pltpu.make_async_remote_copy(
                src_ref=bufs[matrix].at[where], dst_ref=bufs[matrix].at[where],
                send_sem=send_sem.at[slot], recv_sem=recv_sem.at[slot],
                device_id=(peers[axis],), device_id_type=MESH))
        return out

    def start(piece, phase):
        for copy in copies(piece, phase):
            copy.start()

    def arrived(piece, phase):
        for copy in copies(piece, phase):
            copy.wait_recv()

    def second(piece):
        arrived(piece, 0)
        start(piece, 1)

    def third(piece):
        arrived(piece, 1)
        start(piece, 2)
        start(piece, 3)

    def hand_over(piece):
        arrived(piece, 2)
        start(piece, 4)

    def complete(piece):
        arrived(piece, 3)
        arrived(piece, 4)

    def load(matrix):
        return pltpu.make_async_copy(shards[matrix], bufs[matrix].at[tuple(bits)], load_sem.at[matrix])

    barrier = pltpu.get_barrier_semaphore()
    for peer in peers:
        pl.semaphore_signal(barrier, inc=1, device_id=(peer,), device_id_type=MESH)
    for matrix in range(3):
        load(matrix).start()
    load_x = pltpu.make_async_copy(x_hbm, h_buf, load_sem.at[4])
    load_x.start()
    load(0).wait()
    pl.semaphore_wait(barrier, 4)
    start(0, 0)
    start(1, 0)
    load(1).wait()
    load(2).wait()
    second(0)
    start(2, 0)
    second(1)
    third(0)
    second(2)
    start(3, 0)
    third(1)
    hand_over(0)
    load_x.wait()
    complete(0)

    def weights(matrix, block):
        return bufs[matrix][:, :, :, :, pl.ds(pl.multiple_of(block * quarter, quarter), quarter), :].reshape(4 * 4 * quarter, width)

    def run(count, matrix, body, events):
        def step(index, carry):
            for when, event in events.items():
                pl.when(index == when)(event)
            body(index, matrix)
            return carry
        lax.fori_loop(0, count, step, 0)

    def up(index, matrix):
        block, tile = index // n_tiles, lax.rem(index, n_tiles)
        span = pl.ds(pl.multiple_of(tile * TILE, TILE), TILE)
        pre = jnp.dot(h_buf[span, :], weights(matrix, block), preferred_element_type=jnp.float32)
        gate = 0.5 + 0.5 * jnp.tanh(pre * (GELU_A + GELU_B * (pre * pre)))
        act_buf[block, span, :] = (pre * gate).astype(jnp.bfloat16)

    def down(tile, matrix):
        span = pl.ds(pl.multiple_of(tile * TILE, TILE), TILE)
        total = h_buf[span, :].astype(jnp.float32)
        for block in range(4):
            total = total + jnp.dot(act_buf[block, span, :], bufs[matrix][block // 2, block % 2].reshape(width, width), preferred_element_type=jnp.float32)
        h_buf[span, :] = total.astype(jnp.bfloat16)

    def store(tile):
        span = pl.ds(pl.multiple_of(tile * TILE, TILE), TILE)
        return pltpu.make_async_copy(h_buf.at[span, :], y_hbm.at[span, :], load_sem.at[5 + tile])

    def down_last(tile, matrix):
        down(tile, matrix)
        store(tile).start()

    def widen_both():
        second(3)
        third(2)

    run(4 * n_tiles, 0, up, {3: widen_both, 2 * n_tiles - 3: lambda: hand_over(1), 2 * n_tiles: lambda: complete(1),
                             3 * n_tiles: lambda: third(3), 4 * n_tiles - 1: lambda: hand_over(2)})
    for piece in (0, 1):
        for phase in range(5):
            for copy in copies(piece, phase):
                copy.wait_send()
    for peer in peers:
        pl.semaphore_signal(free_sem, inc=1, device_id=(peer,), device_id_type=MESH)
    load(3).start()
    complete(2)
    load(3).wait()
    pl.semaphore_wait(free_sem, 4)
    start(4, 0)
    run(n_tiles, 1, down, {n_tiles - 2: lambda: hand_over(3), n_tiles - 1: lambda: second(4)})
    complete(3)
    run(4 * n_tiles, 2, up, {n_tiles: lambda: third(4), 4 * n_tiles - 2: lambda: hand_over(4)})
    complete(4)
    run(n_tiles, 3, down_last, {})
    for piece in (2, 3, 4):
        for phase in range(5):
            for copy in copies(piece, phase):
                copy.wait_send()
    for tile in range(n_tiles):
        store(tile).wait()


def forward_stack(x_tokens, up_shard, down_shard, n_dev):
    tokens, model_width = x_tokens.shape
    layers, rows, ff_width = up_shard.shape
    blocks = ff_width // model_width
    up_blocks = up_shard.reshape(layers, rows, blocks, model_width).transpose(0, 2, 1, 3).reshape(layers, blocks * rows, model_width)
    hbm = pl.BlockSpec(memory_space=pl.ANY)
    b16 = jnp.bfloat16
    gathered = pltpu.VMEM((2, 2, 2, 2, blocks * rows, model_width), b16)
    dma = pltpu.SemaphoreType.DMA
    return pl.pallas_call(
        forward_kernel, in_specs=[hbm] * 5, out_specs=hbm,
        out_shape=jax.ShapeDtypeStruct((tokens, model_width), b16),
        scratch_shapes=[pltpu.VMEM((tokens, model_width), b16), pltpu.VMEM((blocks, tokens, model_width), b16), gathered, gathered, gathered,
                        dma((5 + tokens // TILE,)), pltpu.SemaphoreType.REGULAR, dma((75,)), dma((75,))],
        compiler_params=pltpu.CompilerParams(vmem_limit_bytes=67_043_328, collective_id=1, has_side_effects=True),
        cost_estimate=pl.CostEstimate(flops=8 * tokens * model_width * ff_width, bytes_accessed=20_000_000, transcendentals=2 * tokens * ff_width),
        name="gather_forward",
    )(x_tokens, up_blocks[0], down_shard[0], up_blocks[1], down_shard[1])


def solution(mesh):
    n_dev = mesh.shape["fsdp"]
    rows_spec = P(None, "fsdp")

    def local_step(x_saved, grad_out, x_next, w_up, w_down, gacc_up, gacc_down, master_up, master_down, mom1_up, mom1_down, mom2_up, mom2_down):
        layers, model_width, ff_width = w_up.shape
        clip_norm = 0.1 * math.sqrt(2 * layers * model_width * ff_width)
        grad_up, grad_down, norm_sq = backward_grads(x_saved.reshape(layers, -1, model_width), grad_out.reshape(-1, model_width), w_up, w_down, gacc_up, gacc_down, n_dev)
        clip_factor = jnp.minimum(1.0, clip_norm / jnp.sqrt(norm_sq))
        new_up = adamw_update(master_up, mom1_up, mom2_up, grad_up * clip_factor)
        new_down = adamw_update(master_down, mom1_down, mom2_down, grad_down * clip_factor)
        up_shard = new_up[0].astype(jnp.bfloat16)
        down_shard = new_down[0].astype(jnp.bfloat16)
        hidden_state = forward_stack(x_next.reshape(-1, model_width), up_shard, down_shard, n_dev)
        return (hidden_state.reshape(x_next.shape), new_up[0], new_down[0], new_up[1], new_down[1], new_up[2], new_down[2])

    return jax.shard_map(local_step, mesh=mesh, in_specs=(rows_spec, P("fsdp"), P("fsdp"), P(), P(), rows_spec, rows_spec, rows_spec, rows_spec, rows_spec, rows_spec, rows_spec, rows_spec), out_specs=(P("fsdp"), rows_spec, rows_spec, rows_spec, rows_spec, rows_spec, rows_spec), check_vma=False)
```

```python
import functools
import math
import jax
import jax.numpy as jnp
from jax import lax
from jax.experimental import pallas as pl
from jax.experimental.pallas import tpu as pltpu
from jax.sharding import PartitionSpec as P

LEARN_RATE = 0.001
BETA_ONE = 0.9
BETA_TWO = 0.95
ADAM_EPS = 1e-8
WEIGHT_DECAY = 0.1
ADAM_STEP = 3

GELU_A = math.sqrt(2.0 / math.pi)
GELU_B = GELU_A * 0.044715
MESH = pl.DeviceIdType.MESH
STRIDES = (8, 4, 2, 1)
ORDERS = ((2, 1, 0), (1, 0, 2), (0, 2, 1))
TILE = 512
LANES = 128
ROWS = 128
TILE_B = 512


def adamw_update(master_old, mom_one, mom_two, grad_clip):
    mom_one_new = BETA_ONE * mom_one + (1.0 - BETA_ONE) * grad_clip
    mom_two_new = BETA_TWO * mom_two + (1.0 - BETA_TWO) * grad_clip * grad_clip
    first_hat = mom_one_new / (1.0 - BETA_ONE ** ADAM_STEP)
    second_hat = mom_two_new / (1.0 - BETA_TWO ** ADAM_STEP)
    master_new = master_old - LEARN_RATE * (first_hat / (jnp.sqrt(second_hat) + ADAM_EPS) + WEIGHT_DECAY * master_old)
    return master_new, mom_one_new, mom_two_new


def dot_nt(left, right):
    return lax.dot_general(left, right, (((1,), (1,)), ((), ())), preferred_element_type=jnp.float32)


def at_bits(picks, count):
    return tuple(picks.get(dim, slice(None)) for dim in range(count))


def backward_kernel(n_steps, n_chunks, cols, x_hbm, g_hbm, w1_hbm, w2_ref, gacc1_hbm, gacc2_ref, out1_block, out2_ref, norm_ref, x_buf, g_buf, x_turned, acc, act_turned, dh_buf, w1_group, w1_ref, w1_next, part1, part2, *rest):
    parts = (part1, part2)
    out1_ref = out1_block.at[0]
    recv0, send1, keep1, recv1, send2, keep2, recv2, send3, keep3, recv3 = (rest[2 * i:2 * i + 2] for i in range(10))
    squares, gathered, load_sem, group_sem, send_sem0, recv_sem0, send_sem, recv_sem, norm_send, norm_recv = rest[20:]
    step = pl.program_id(0)
    me = lax.axis_index("fsdp")
    bits = [lax.rem(me // stride, 2) for stride in STRIDES]
    peers = [me + (1 - 2 * bit) * stride for bit, stride in zip(bits, STRIDES)]
    tokens = x_buf.shape[0]
    sends = (send1, send2, send3)
    recvs = (recv1, recv2, recv3)

    def core_copy(mat, block):
        return pltpu.make_async_remote_copy(
            src_ref=parts[mat].at[:, :, :, 1 - bits[3]], dst_ref=recv0[mat].at[lax.rem(block, 2)],
            send_sem=send_sem0.at[mat], recv_sem=recv_sem0.at[mat, lax.rem(block, 2)],
            device_id=(peers[3],), device_id_type=MESH)

    def axis_copy(phase, mat, color, block):
        lo, hi = cols[mat][color]
        lead = (slice(None),) * (4 - phase)
        slot = (phase - 1) * 6 + mat * 3 + color
        return pltpu.make_async_remote_copy(
            src_ref=sends[phase - 1][mat].at[lead + (pl.ds(lo, hi - lo),)],
            dst_ref=recvs[phase - 1][mat].at[(lax.rem(block, 2),) + lead + (pl.ds(lo, hi - lo),)],
            send_sem=send_sem.at[slot], recv_sem=recv_sem.at[slot, lax.rem(block, 2)],
            device_id=(peers[ORDERS[color][phase - 1]],), device_id_type=MESH)

    def colors(mat):
        return [(color, pl.ds(lo, hi - lo)) for color, (lo, hi) in enumerate(cols[mat])]

    n_dev, per_dev = w2_ref.shape[:2]
    spread = LANES // per_dev

    def lane_part():
        return lax.broadcasted_iota(jnp.int32, (ROWS, LANES), 1) // per_dev

    def group_copies(layer, half):
        return [pltpu.make_async_copy(
            w1_hbm.at[layer, :, pl.ds(pl.multiple_of((dev * n_chunks // spread + half) * LANES, LANES), LANES)],
            w1_group.at[dev], group_sem.at[dev]) for dev in range(n_dev)]

    def order_columns(rows, phase, target):
        part = lane_part()
        for tile in range(n_dev // spread):
            merged = None
            for place in range(spread):
                moved = w1_group[tile * spread + place, rows, :].astype(jnp.float32)
                moved = pltpu.roll(moved, lax.rem(place - phase + spread, spread) * per_dev, 1)
                merged = moved if merged is None else jnp.where(part == place, moved, merged)
            target[rows, tile * LANES:(tile + 1) * LANES] = merged.astype(jnp.bfloat16)

    @pl.when(step == 0)
    def _():
        for copy in group_copies(w1_hbm.shape[0] - 1, 0):
            copy.start()
        load_x = pltpu.make_async_copy(x_hbm.at[w1_hbm.shape[0] - 1], x_buf, load_sem.at[0])
        load_g = pltpu.make_async_copy(g_hbm, g_buf, load_sem.at[1])
        load_x.start()
        load_g.start()
        barrier = pltpu.get_barrier_semaphore()
        for shift in range(1, n_dev):
            pl.semaphore_signal(barrier, inc=1, device_id=(lax.rem(me + shift, n_dev),), device_id_type=MESH)
        acc[...] = jnp.zeros_like(acc)
        squares[...] = jnp.zeros_like(squares)
        for copy in group_copies(0, 0):
            copy.wait()

        def row_body(block, carry):
            order_columns(pl.ds(pl.multiple_of(block * ROWS, ROWS), ROWS), 0, w1_next)
            return carry
        lax.fori_loop(0, x_buf.shape[1] // ROWS, row_body, 0)
        load_x.wait()
        load_g.wait()
        pl.semaphore_wait(barrier, n_dev - 1)

    def next_x():
        return pltpu.make_async_copy(x_hbm.at[0], x_buf, load_sem.at[0])

    @pl.when(step == n_chunks)
    def _():
        next_x().wait()

    def add_squares(grad):
        total = squares[...]
        for row in range(0, grad.shape[0], 8):
            for lane in range(0, grad.shape[1], LANES):
                piece = grad[row:row + 8, lane:lane + LANES]
                total = total + piece * piece
        squares[...] = total

    def advance(mat):
        @pl.when(step >= 4)
        def _():
            block = step - 4
            for color, span in colors(mat):
                copy = axis_copy(3, mat, color, block)
                copy.wait_send()
                copy.wait_recv()
                total = keep3[mat][:, span] + recv3[mat][lax.rem(block, 2), :, span]
                if mat == 1:
                    grad = 0.5 * (gacc2_ref[:, span] + total)
                    out2_ref[:, span] = grad
                    add_squares(grad)
                else:
                    keep3[0][:, span] = total
            if mat == 1:
                return
            chunk = lax.rem(block, n_chunks)

            @pl.when(chunk == 0)
            def _():
                load = pltpu.make_async_copy(gacc1_hbm.at[w1_hbm.shape[0] - 1 - block // n_chunks], out1_ref, load_sem.at[2])
                load.start()
                load.wait()
            phase = lax.rem(chunk, spread)
            part = lax.broadcasted_iota(jnp.int32, (out1_ref.shape[0], LANES), 1) // per_dev
            for dev in range(n_dev):
                tile = dev // spread
                moved = pltpu.roll(keep3[0][:, tile * LANES:(tile + 1) * LANES], lax.rem(phase - dev % spread + spread, spread) * per_dev, 1)
                spot = pl.ds(pl.multiple_of((dev * n_chunks // spread + chunk // spread) * LANES, LANES), LANES)
                out1_ref[:, spot] = jnp.where(part == phase, 0.5 * (out1_ref[:, spot] + moved), out1_ref[:, spot])

            @pl.when(chunk == n_chunks - 1)
            def _():
                add_squares(out1_ref[...])

        @pl.when((step >= 3) & (step < n_steps + 3))
        def _():
            block = step - 3
            for color, span in colors(mat):
                copy = axis_copy(2, mat, color, block)
                copy.wait_send()
                copy.wait_recv()
                bit = bits[ORDERS[color][2]]
                slot = lax.rem(block, 2)
                send3[mat][:, span] = keep2[mat][1 - bit, :, span] + recv2[mat][slot, 1 - bit, :, span]
                keep3[mat][:, span] = keep2[mat][bit, :, span] + recv2[mat][slot, bit, :, span]
                axis_copy(3, mat, color, block).start()

        @pl.when((step >= 2) & (step < n_steps + 2))
        def _():
            block = step - 2
            for color, span in colors(mat):
                copy = axis_copy(1, mat, color, block)
                copy.wait_send()
                copy.wait_recv()
                left = [axis for axis in range(3) if axis != ORDERS[color][0]]
                place = left.index(ORDERS[color][1])
                bit = bits[ORDERS[color][1]]
                slot = lax.rem(block, 2)
                for value, store in ((1 - bit, send2), (bit, keep2)):
                    index = at_bits({place: value}, 2)
                    store[mat][:, :, span] = keep1[mat][index + (slice(None), span)] + recv1[mat][(slot,) + index + (slice(None), span)]
                axis_copy(2, mat, color, block).start()

        @pl.when((step >= 1) & (step < n_steps + 1))
        def _():
            block = step - 1
            copy = core_copy(mat, block)
            copy.wait_send()
            copy.wait_recv()
            for color, span in colors(mat):
                axis = ORDERS[color][0]
                slot = lax.rem(block, 2)
                for value, store in ((1 - bits[axis], send1), (bits[axis], keep1)):
                    index = at_bits({axis: value}, 3)
                    mine = parts[mat][index + (bits[3], slice(None), span)].astype(jnp.float32)
                    store[mat][:, :, :, span] = mine + recv0[mat][(slot,) + index + (slice(None), span)].astype(jnp.float32)
                axis_copy(1, mat, color, block).start()

    advance(0)

    @pl.when(step < n_steps)
    def _():
        w1_ref[...] = w1_next[...]

    @pl.when((step < n_steps - 1) & (lax.rem(step, spread) == spread - 1))
    def _():
        for copy in group_copies(0, 0):
            copy.wait()

    def tile_body(tile, turn_x):
        rows = pl.ds(pl.multiple_of(tile * TILE_B, TILE_B), TILE_B)
        pre = jnp.dot(x_buf[rows, :], w1_ref[...], preferred_element_type=jnp.float32)
        d_act = dot_nt(g_buf[rows, :], w2_ref[...].reshape(w1_ref.shape[1], w1_ref.shape[0]))
        square = pre * pre
        gate = 0.5 + 0.5 * jnp.tanh(pre * (GELU_A + GELU_B * square))
        act = pre * gate
        act_turned[:, rows] = act.astype(jnp.bfloat16).T
        slope = gate + (act * (1.0 - gate)) * (2.0 * GELU_A + 6.0 * GELU_B * square)
        dh_buf[rows, :] = (d_act * slope).astype(jnp.bfloat16)
        if turn_x:
            x_turned[:, rows] = x_buf[rows, :].T

    first = lax.rem(step, n_chunks) == 0

    @pl.when((step < n_steps) & first)
    def _():
        lax.fori_loop(0, tokens // TILE_B, lambda tile, carry: (tile_body(tile, True), carry)[1], 0)

    @pl.when((step < n_steps) & (lax.rem(step, n_chunks) > 0))
    def _():
        lax.fori_loop(0, tokens // TILE_B, lambda tile, carry: (tile_body(tile, False), carry)[1], 0)

    @pl.when(step < n_steps)
    def _():
        for block in range(w1_next.shape[0] // ROWS):
            order_columns(pl.ds(block * ROWS, ROWS), lax.rem(step + 1, spread), w1_next)
        part1[...] = jnp.dot(x_turned[...], dh_buf[...], preferred_element_type=jnp.float32).astype(jnp.bfloat16).reshape(part1.shape)
        core_copy(0, step).start()

    @pl.when(step == n_chunks - 1)
    def _():
        next_x().start()

    @pl.when((step < n_steps - 2) & (lax.rem(step, spread) == spread - 2))
    def _():
        following = step + 2
        for copy in group_copies(w1_hbm.shape[0] - 1 - following // n_chunks, lax.rem(following, n_chunks) // spread):
            copy.start()

    advance(1)

    @pl.when(step < n_steps)
    def _():
        part2[...] = jnp.dot(act_turned[...], g_buf[...], preferred_element_type=jnp.float32).astype(jnp.bfloat16).reshape(part2.shape)
        core_copy(1, step).start()

    @pl.when(step < n_chunks)
    def _():
        def tile_body(tile, carry):
            rows = pl.ds(pl.multiple_of(tile * TILE, TILE), TILE)
            acc[rows, :] += dot_nt(dh_buf[rows, :], w1_ref[...])
            return carry
        lax.fori_loop(0, tokens // TILE, tile_body, 0)

    @pl.when(step == n_chunks - 1)
    def _():
        def tile_body(tile, carry):
            rows = pl.ds(pl.multiple_of(tile * TILE, TILE), TILE)
            g_buf[rows, :] = (g_buf[rows, :].astype(jnp.float32) + acc[rows, :]).astype(jnp.bfloat16)
            return carry
        lax.fori_loop(0, tokens // TILE, tile_body, 0)

    @pl.when(step == n_steps + 3)
    def _():
        def copy_of(shift, sender):
            return pltpu.make_async_remote_copy(
                src_ref=squares, dst_ref=gathered.at[sender], send_sem=norm_send.at[shift], recv_sem=norm_recv.at[sender],
                device_id=(lax.rem(me + shift, n_dev),), device_id_type=MESH)

        for shift in range(1, n_dev):
            copy_of(shift, me).start()
        gathered[me] = squares[...]
        for shift in range(1, n_dev):
            copy_of(shift, lax.rem(me + n_dev - shift, n_dev)).wait_recv()
        total = gathered[0]
        for dev in range(1, n_dev):
            total = total + gathered[dev]
        norm_ref[...] = jnp.broadcast_to(jnp.sum(total, keepdims=True), norm_ref.shape)
        for shift in range(1, n_dev):
            copy_of(shift, me).wait_send()


def backward_grads(x_tokens, grad_tokens, w_up, w_down, gacc_up, gacc_down, n_dev):
    layers, model_width, ff_width = w_up.shape
    tokens = grad_tokens.shape[0]
    chunk = 512
    n_chunks = ff_width // chunk
    per_dev = chunk // n_dev
    rows_up = model_width // n_dev
    n_steps = layers * n_chunks
    cols = (((0, chunk // 4), (chunk // 4, chunk // 2), (chunk // 2, chunk)), ((0, 384), (384, 768), (768, model_width)))
    w2_view = w_down.reshape(layers, n_dev, n_chunks, per_dev, model_width)

    def where(step):
        last = jnp.minimum(step, n_steps - 1)
        return layers - 1 - last // n_chunks, lax.rem(last, n_chunks)

    def pair(lead, dtype):
        return [pltpu.VMEM(lead + (rows_up, chunk), dtype), pltpu.VMEM(lead + (per_dev, model_width), dtype)]

    f32, b16 = jnp.float32, jnp.bfloat16
    scratch = [pltpu.VMEM((tokens, model_width), b16), pltpu.VMEM((tokens, model_width), b16), pltpu.VMEM((model_width, tokens), b16),
               pltpu.VMEM((tokens, model_width), f32), pltpu.VMEM((chunk, tokens), b16), pltpu.VMEM((tokens, chunk), b16),
               pltpu.VMEM((n_dev, model_width, LANES), b16), pltpu.VMEM((model_width, chunk), b16), pltpu.VMEM((model_width, chunk), b16)]
    scratch += pair((2, 2, 2, 2), b16) + pair((2, 2, 2, 2), b16)
    for lead in ((2, 2), (2,), ()):
        scratch += pair(lead, f32) + pair(lead, f32) + pair((2,) + lead, f32)
    dma = pltpu.SemaphoreType.DMA
    scratch += [pltpu.VMEM((8, LANES), f32), pltpu.VMEM((n_dev, 8, LANES), f32)]
    scratch += [dma((3,)), dma((n_dev,)), dma((2,)), dma((2, 2)), dma((18,)), dma((18, 2)), dma((n_dev,)), dma((n_dev,))]
    hbm = pl.BlockSpec(memory_space=pl.ANY)
    grad_up, grad_down, norm_sq = pl.pallas_call(
        functools.partial(backward_kernel, n_steps, n_chunks, cols),
        grid=(n_steps + 4,),
        in_specs=[hbm, hbm,
                  hbm,
                  pl.BlockSpec((None, n_dev, None, per_dev, model_width), lambda s: (where(s)[0], 0, where(s)[1], 0, 0)),
                  hbm, pl.BlockSpec((None, per_dev, model_width), lambda s: (*where(jnp.maximum(s - 4, 0)), 0))],
        out_specs=[pl.BlockSpec((1, rows_up, ff_width), lambda s: (where(jnp.maximum(s - 4, 0))[0], 0, 0)),
                   pl.BlockSpec((None, per_dev, model_width), lambda s: (*where(jnp.maximum(s - 4, 0)), 0)),
                   pl.BlockSpec((8, LANES), lambda s: (0, 0))],
        out_shape=[jax.ShapeDtypeStruct((layers, rows_up, ff_width), f32), jax.ShapeDtypeStruct((layers, n_chunks * per_dev, model_width), f32),
                   jax.ShapeDtypeStruct((8, LANES), f32)],
        scratch_shapes=scratch,
        compiler_params=pltpu.CompilerParams(vmem_limit_bytes=67_043_328, dimension_semantics=("arbitrary",), collective_id=0, has_side_effects=True),
        cost_estimate=pl.CostEstimate(flops=18 * tokens * model_width * ff_width, bytes_accessed=60_000_000, transcendentals=2 * tokens * ff_width),
        name="backward_reduce",
    )(x_tokens, grad_tokens, w_up, w2_view, gacc_up, gacc_down)
    return grad_up, grad_down, norm_sq[0, 0]


def forward_kernel(x_hbm, up0_hbm, down0_hbm, up1_hbm, down1_hbm, y_hbm, h_buf, act_buf, buf_a, buf_b, buf_c, load_sem, free_sem, send_sem, recv_sem):
    shards = (up0_hbm, down0_hbm, up1_hbm, down1_hbm)
    bufs = (buf_a, buf_b, buf_c, buf_a)
    me = lax.axis_index("fsdp")
    bits = [lax.rem(me // stride, 2) for stride in STRIDES]
    peers = [me + (1 - 2 * bit) * stride for bit, stride in zip(bits, STRIDES)]
    rows = up0_hbm.shape[0]
    tokens, width = h_buf.shape
    quarter = rows // 4
    pieces = ((0, 0, rows // 2), (0, rows // 2, rows), (1, 0, rows), (2, 0, rows), (3, 0, rows))
    n_tiles = tokens // TILE

    def spans(piece):
        _, lo, hi = pieces[piece]
        third = (hi - lo) // 48 * 16
        rest = lo + 3 * third
        cuts = (0, 3 * width // 8, 3 * width // 4, width)
        return ([(color, lo + color * third, third, 0, width) for color in range(3)]
                + [(color, rest, hi - rest, cuts[color], cuts[color + 1] - cuts[color]) for color in range(3)])

    def copies(piece, phase):
        matrix = pieces[piece][0]
        out = []
        for index, (color, lo, size, left, breadth) in enumerate(spans(piece)):
            order = ORDERS[color]
            picks = {axis: bits[axis] for axis in range(4)}
            for axis in order[:min(phase, 2)]:
                picks.pop(axis)
            if phase == 4:
                picks[order[2]] = 1 - bits[order[2]]
            where = at_bits(picks, 4) + (pl.ds(lo, size), pl.ds(left, breadth))
            axis = order[phase] if phase < 3 else 3
            slot = (piece * 5 + phase) * 6 + index
            out.append(pltpu.make_async_remote_copy(
                src_ref=bufs[matrix].at[where], dst_ref=bufs[matrix].at[where],
                send_sem=send_sem.at[slot], recv_sem=recv_sem.at[slot],
                device_id=(peers[axis],), device_id_type=MESH))
        return out

    def start(piece, phase):
        for copy in copies(piece, phase):
            copy.start()

    def arrived(piece, phase):
        for copy in copies(piece, phase):
            copy.wait_recv()

    def second(piece):
        arrived(piece, 0)
        start(piece, 1)

    def third(piece):
        arrived(piece, 1)
        start(piece, 2)
        start(piece, 3)

    def hand_over(piece):
        arrived(piece, 2)
        start(piece, 4)

    def complete(piece):
        arrived(piece, 3)
        arrived(piece, 4)

    def load(matrix):
        return pltpu.make_async_copy(shards[matrix], bufs[matrix].at[tuple(bits)], load_sem.at[matrix])

    barrier = pltpu.get_barrier_semaphore()
    for peer in peers:
        pl.semaphore_signal(barrier, inc=1, device_id=(peer,), device_id_type=MESH)
    for matrix in range(3):
        load(matrix).start()
    load_x = pltpu.make_async_copy(x_hbm, h_buf, load_sem.at[4])
    load_x.start()
    load(0).wait()
    pl.semaphore_wait(barrier, 4)
    start(0, 0)
    start(1, 0)
    load(1).wait()
    load(2).wait()
    second(0)
    start(2, 0)
    second(1)
    third(0)
    second(2)
    start(3, 0)
    third(1)
    hand_over(0)
    load_x.wait()
    complete(0)

    def weights(matrix, block):
        return bufs[matrix][:, :, :, :, pl.ds(pl.multiple_of(block * quarter, quarter), quarter), :].reshape(4 * 4 * quarter, width)

    def run(count, matrix, body, events):
        def step(index, carry):
            for when, event in events.items():
                pl.when(index == when)(event)
            body(index, matrix)
            return carry
        lax.fori_loop(0, count, step, 0)

    def up(index, matrix):
        block, tile = index // n_tiles, lax.rem(index, n_tiles)
        span = pl.ds(pl.multiple_of(tile * TILE, TILE), TILE)
        pre = jnp.dot(h_buf[span, :], weights(matrix, block), preferred_element_type=jnp.float32)
        gate = 0.5 + 0.5 * jnp.tanh(pre * (GELU_A + GELU_B * (pre * pre)))
        act_buf[block, span, :] = (pre * gate).astype(jnp.bfloat16)

    def down(tile, matrix):
        span = pl.ds(pl.multiple_of(tile * TILE, TILE), TILE)
        total = h_buf[span, :].astype(jnp.float32)
        for block in range(4):
            total = total + jnp.dot(act_buf[block, span, :], bufs[matrix][block // 2, block % 2].reshape(width, width), preferred_element_type=jnp.float32)
        h_buf[span, :] = total.astype(jnp.bfloat16)

    def store(tile):
        span = pl.ds(pl.multiple_of(tile * TILE, TILE), TILE)
        return pltpu.make_async_copy(h_buf.at[span, :], y_hbm.at[span, :], load_sem.at[5 + tile])

    def down_last(tile, matrix):
        down(tile, matrix)
        store(tile).start()

    def widen_both():
        second(3)
        third(2)

    run(4 * n_tiles, 0, up, {3: widen_both, 2 * n_tiles - 3: lambda: hand_over(1), 2 * n_tiles: lambda: complete(1),
                             3 * n_tiles: lambda: third(3), 4 * n_tiles - 1: lambda: hand_over(2)})
    for piece in (0, 1):
        for phase in range(5):
            for copy in copies(piece, phase):
                copy.wait_send()
    for peer in peers:
        pl.semaphore_signal(free_sem, inc=1, device_id=(peer,), device_id_type=MESH)
    load(3).start()
    complete(2)
    load(3).wait()
    pl.semaphore_wait(free_sem, 4)
    start(4, 0)
    run(n_tiles, 1, down, {n_tiles - 2: lambda: hand_over(3), n_tiles - 1: lambda: second(4)})
    complete(3)
    run(4 * n_tiles, 2, up, {n_tiles: lambda: third(4), 4 * n_tiles - 2: lambda: hand_over(4)})
    complete(4)
    run(n_tiles, 3, down_last, {})
    for piece in (2, 3, 4):
        for phase in range(5):
            for copy in copies(piece, phase):
                copy.wait_send()
    for tile in range(n_tiles):
        store(tile).wait()


def forward_stack(x_tokens, up_shard, down_shard, n_dev):
    tokens, model_width = x_tokens.shape
    layers, rows, ff_width = up_shard.shape
    blocks = ff_width // model_width
    up_blocks = up_shard.reshape(layers, rows, blocks, model_width).transpose(0, 2, 1, 3).reshape(layers, blocks * rows, model_width)
    hbm = pl.BlockSpec(memory_space=pl.ANY)
    b16 = jnp.bfloat16
    gathered = pltpu.VMEM((2, 2, 2, 2, blocks * rows, model_width), b16)
    dma = pltpu.SemaphoreType.DMA
    return pl.pallas_call(
        forward_kernel, in_specs=[hbm] * 5, out_specs=hbm,
        out_shape=jax.ShapeDtypeStruct((tokens, model_width), b16),
        scratch_shapes=[pltpu.VMEM((tokens, model_width), b16), pltpu.VMEM((blocks, tokens, model_width), b16), gathered, gathered, gathered,
                        dma((5 + tokens // TILE,)), pltpu.SemaphoreType.REGULAR, dma((150,)), dma((150,))],
        compiler_params=pltpu.CompilerParams(vmem_limit_bytes=67_043_328, collective_id=1, has_side_effects=True),
        cost_estimate=pl.CostEstimate(flops=8 * tokens * model_width * ff_width, bytes_accessed=20_000_000, transcendentals=2 * tokens * ff_width),
        name="gather_forward",
    )(x_tokens, up_blocks[0], down_shard[0], up_blocks[1], down_shard[1])


def solution(mesh):
    n_dev = mesh.shape["fsdp"]
    rows_spec = P(None, "fsdp")

    def local_step(x_saved, grad_out, x_next, w_up, w_down, gacc_up, gacc_down, master_up, master_down, mom1_up, mom1_down, mom2_up, mom2_down):
        layers, model_width, ff_width = w_up.shape
        clip_norm = 0.1 * math.sqrt(2 * layers * model_width * ff_width)
        grad_up, grad_down, norm_sq = backward_grads(x_saved.reshape(layers, -1, model_width), grad_out.reshape(-1, model_width), w_up, w_down, gacc_up, gacc_down, n_dev)
        clip_factor = jnp.minimum(1.0, clip_norm / jnp.sqrt(norm_sq))
        new_up = adamw_update(master_up, mom1_up, mom2_up, grad_up * clip_factor)
        new_down = adamw_update(master_down, mom1_down, mom2_down, grad_down * clip_factor)
        up_shard = new_up[0].astype(jnp.bfloat16)
        down_shard = new_down[0].astype(jnp.bfloat16)
        hidden_state = forward_stack(x_next.reshape(-1, model_width), up_shard, down_shard, n_dev)
        return (hidden_state.reshape(x_next.shape), new_up[0], new_down[0], new_up[1], new_down[1], new_up[2], new_down[2])

    return jax.shard_map(local_step, mesh=mesh, in_specs=(rows_spec, P("fsdp"), P("fsdp"), P(), P(), rows_spec, rows_spec, rows_spec, rows_spec, rows_spec, rows_spec, rows_spec, rows_spec), out_specs=(P("fsdp"), rows_spec, rows_spec, rows_spec, rows_spec, rows_spec, rows_spec), check_vma=False)
```
